256 devices in a mesh: dp: 64 (over y, z, core), grp: 4 (over x).
Axes of the slice: x: 4, y: 4, z: 8, core: 2. Of those that a mesh axis runs over, the one named last changes fastest.
Arguments:
- vectors: bfloat16 [262144, 1024], P('dp', 'grp'), may hold values from -6 to 6
- coarse_init: float32 [1024, 1024], P(None, 'grp'), may hold values from -4 to 4
- fine_init: float32 [1024, 64, 1024], P('dp', None, 'grp'), may hold values from -4 to 4
- owner_of: int32 [262144, 1], P('dp'), may hold values from 0 to 63; in each aligned block of 4096 rows (0 to 4095, 4096 to 8191, ...) at most 128 rows name the same one
- slot_in_owner: int32 [262144], P('dp'), may hold values from 0 to 15
- fine_in_cluster: int32 [262144], P('dp'), may hold values from 0 to 63
- slot_cluster: int32 [1024], replicated, may hold values from 0 to 1023, each once
Outputs:
- coarse_out: float32 [1024, 1024], P(None, 'grp')
- fine_out: float32 [1024, 64, 1024], P('dp', None, 'grp')
- distances: float32 [64, 262144], P(None, 'dp')
The draws below stay inside these ranges and needn't reach their ends.
Inputs may be any that keep to these rules, and one draw needn't show every extreme that they name: Among the 4096 vectors of one dp index at most 128 have the same owner_of, a bound that some block reaches of them. `slot_cluster`: each coarse cluster stands in exactly one slot.
All inputs are finite; a program needn't handle non-finite values.
Results may differ from the reference program's by a relative error of at most 0.0003.
Values may be sent and summed in bfloat16 or wider, within the bound.
No kernel may reach another device: no remote copies, remote signals or barrier semaphores. Data moves between devices by JAX's collectives and lax.ppermute only.
A program may use at most 64 MiB of HBM per device.

```python
import math
import jax
import jax.numpy as jnp
import numpy as np
from jax import lax

D = 1024
KC = 1024
FPC = 64
PASSES = 2
TOK_DEV = 4096
SLOTS = 16
OWN_CAP = 128
NVEC = 262144
N_DP = 64


def plant(entries, key, smallest, high):
    dims = entries.shape
    index_at = [jax.random.randint(jax.random.fold_in(key, axis), (), 0, dims[axis]) for axis in range(len(dims))]
    entries = entries.at[tuple(index_at)].set(smallest)
    longest = dims.index(max(dims))
    index_at[longest] = (index_at[longest] + 1) % dims[longest]
    return entries.at[tuple(index_at)].set(high)


def steps_of(rng, extent, pieces, smallest, top_value):
    def one(position, blocks):
        steps = jax.random.uniform(jax.random.fold_in(jax.random.fold_in(rng, 6), position), (blocks,), jnp.float32, smallest / len(pieces), top_value / len(pieces))
        return jnp.repeat(jnp.exp(steps), extent[position] // blocks).reshape((-1,) + (1,) * (len(extent) - position - 1))

    level = one(*pieces[0])
    for cut in pieces[1:]:
        level = level * one(*cut)
    return level


def routed_block(key, own, number, rows, amount, top, most, slope):
    sequence = jax.random.permutation(key, amount)
    packed, common = portions_of(amount, rows * top, most, slope, True), portions_of(amount, rows * top, most, slope, False)
    places = jnp.arange(amount)

    def named(lengths, offset_by):
        used = int((lengths > 0).sum())
        fixed = max(1, used // 4)
        shifted = fixed + (places - fixed + offset_by * (used - fixed)) % max(1, amount - fixed)
        return jnp.zeros((amount,), jnp.int32).at[sequence[jnp.where(places < fixed, places, shifted)]].set(jnp.asarray(lengths, jnp.int32))

    lengths = jnp.where(number % 4 == 0, named(packed, number // 4), named(common, number - number // 4 - 1))
    mixed = jax.random.permutation(jax.random.fold_in(own, 3), amount)
    donor, taker = mixed[0:amount // 2 * 2:2], mixed[1:amount // 2 * 2:2]
    slack = jnp.minimum(lengths[donor] - 1, most - lengths[taker]) // 2
    slack = jnp.where((donor == sequence[0]) | (taker == sequence[0]) | (lengths[taker] == 0), 0, jnp.maximum(slack, 0))
    shifted = jax.random.randint(jax.random.fold_in(own, 4), (amount // 2,), 0, 1 << 20) % (slack + 1)
    lengths = lengths.at[donor].add(-shifted).at[taker].add(shifted)
    members = jnp.searchsorted(jnp.cumsum(lengths), jnp.arange(rows * top), side="right").astype(jnp.int32)
    listing = members.reshape(top, rows).T
    listing = listing[jax.random.permutation(jax.random.fold_in(own, 1), rows)]
    offset_by = jax.random.randint(jax.random.fold_in(own, 2), (rows, 1), 0, top)
    return jnp.take_along_axis(listing, (jnp.arange(top)[None, :] + offset_by) % top, axis=1)


def portions_of(number_of, total, reach, slope, full):
    weights = [(1 << 20) // math.isqrt(standing ** slope) + 1 for standing in range(1, number_of + 1)]
    largest = reach if full else min(reach, max(-(-total // number_of), total * weights[0] // sum(weights)))
    least = 1 if total - largest >= number_of - 1 else 0
    holding, surplus = [largest] + [least] * (number_of - 1), total - largest - least * (number_of - 1)
    while surplus > 0:
        free = [i for i in range(1, number_of) if holding[i] < largest] or [i for i in range(1, number_of) if holding[i] < reach]
        mass, left = sum([weights[i] for i in free]), surplus
        for i in free:
            more = min(reach - holding[i], max(1, left * weights[i] // mass), surplus)
            holding[i] = holding[i] + more
            surplus = surplus - more
    return np.array(holding)


def normal_values(own_key, shape, spread, limit, shards=(), dtype=jnp.bfloat16):
    result = spread * jax.random.normal(own_key, shape, jnp.float32)
    if shards:
        result = result * steps_of(own_key, shape, shards, -0.22, 0.18)
    return jnp.clip(result, -limit, limit).astype(dtype)


def setup_inputs(seed: int = 0) -> dict:
    streams_of = jax.random.split(jax.random.key(seed), 8)
    vectors = normal_values(streams_of[0], (NVEC, D), 1.0, 6.0, ((0, 64), (1, 4)))
    coarse_init = normal_values(streams_of[1], (KC, D), 0.5, 4.0, ((1, 4),), jnp.float32)
    fine_init = normal_values(streams_of[2], (KC, FPC, D), 0.5, 4.0, ((0, 64), (2, 4)), jnp.float32)
    owner_of_keys = jax.random.split(jax.random.fold_in(streams_of[3], 1), NVEC // TOK_DEV)
    owner_of_turns = jax.random.permutation(jax.random.fold_in(streams_of[3], 3), NVEC // TOK_DEV)
    owner_of = jax.vmap(lambda own, number: routed_block(jax.random.fold_in(streams_of[3], 2), own, number, TOK_DEV, N_DP, 1, OWN_CAP, 1))(owner_of_keys, owner_of_turns).reshape((NVEC, 1))
    slot_in_owner = plant(jax.random.randint(streams_of[4], (NVEC,), 0, SLOTS), jax.random.fold_in(streams_of[4], 1), 0, SLOTS - 1).astype(jnp.int32)
    fine_in_cluster = plant(jax.random.randint(streams_of[5], (NVEC,), 0, FPC), jax.random.fold_in(streams_of[5], 1), 0, FPC - 1).astype(jnp.int32)
    slot_cluster = jax.random.permutation(streams_of[6], KC).astype(jnp.int32)
    return {"vectors": vectors, "coarse_init": coarse_init, "fine_init": fine_init, "owner_of": owner_of, "slot_in_owner": slot_in_owner, "fine_in_cluster": fine_in_cluster, "slot_cluster": slot_cluster}


prior_weight = 2.0


def reference(vectors, coarse_init, fine_init, owner_of, slot_in_owner, fine_in_cluster, slot_cluster):
    slot = (owner_of[:, 0] * SLOTS + slot_in_owner).astype(jnp.int32)
    cluster = slot_cluster[slot]
    fine_slot = (slot * FPC + fine_in_cluster).astype(jnp.int32)
    values = vectors.astype(jnp.float32)
    ones = jnp.ones((values.shape[0],), jnp.float32)
    sum_f = jax.ops.segment_sum(values, fine_slot, num_segments=KC * FPC)
    count_f = jax.ops.segment_sum(ones, fine_slot, num_segments=KC * FPC)
    sum_c = jax.ops.segment_sum(values, cluster, num_segments=KC)
    count_c = jax.ops.segment_sum(ones, cluster, num_segments=KC)
    sum_f = sum_f.reshape(KC, FPC, D)
    count_f = count_f.reshape(KC, FPC)
    coarse = coarse_init
    fine = fine_init
    for step in range(PASSES):
        coarse = (sum_c + prior_weight * coarse) / (count_c[:, None] + prior_weight)
        by_slot = coarse[slot_cluster]
        fine = (sum_f - count_f[:, :, None] * by_slot[:, None, :] + prior_weight * fine) / (count_f[:, :, None] + prior_weight)
    by_slot = coarse[slot_cluster]
    cand = (by_slot[:, None, :] + fine).astype(jnp.bfloat16)

    def one_block(args):
        piece, slots_here = args
        chosen = cand[slots_here].astype(jnp.float32)
        diff = piece.astype(jnp.float32)[:, None, :] - chosen
        return jnp.mean(diff * diff, axis=2)

    blocks = values.shape[0] // 512
    dist = lax.map(one_block, (vectors.reshape(blocks, 512, D), slot.reshape(blocks, 512)))
    dist = dist.reshape(-1, FPC)
    return coarse, fine, dist.T
```

```python
import jax
import jax.numpy as jnp
from jax import lax
from jax.experimental import pallas as pl
from jax.experimental.pallas import tpu as pltpu
from jax.sharding import PartitionSpec as P

D = 1024
PASSES = 2
LANES = 128


prior_weight = 2.0

VMEM = pl.BlockSpec(memory_space=pltpu.VMEM)
SMEM = pl.BlockSpec(memory_space=pltpu.SMEM)


def call(body, out_shape, ins, flops, scratch=(), mem=60 << 20):
    return pl.pallas_call(
        body,
        out_shape=out_shape,
        in_specs=ins,
        out_specs=jax.tree.map(lambda _: VMEM, out_shape),
        scratch_shapes=list(scratch),
        compiler_params=pltpu.CompilerParams(vmem_limit_bytes=mem),
        cost_estimate=pl.CostEstimate(flops=flops, bytes_accessed=4 << 20, transcendentals=0),
    )


def exchanged(array, axis):
    return lax.all_to_all(array, axis, split_axis=0, concat_axis=0, tiled=True)


def iota(shape, dim):
    return lax.broadcasted_iota(jnp.int32, shape, dim)


def rank_body(owners, capacity, stride, per_cluster):
    def body(owner_ref, label_ref, target_ref, labels_ref):
        tokens = owner_ref.shape[1]
        step = 256
        upper = (iota((step, step), 0) < iota((step, step), 1)).astype(jnp.bfloat16)
        carry = jnp.zeros((owners, 1), jnp.float32)
        table = jnp.zeros((2 * owners, capacity), jnp.float32)
        for start in range(0, tokens, step):
            owner = owner_ref[:, start : start + step]
            label = label_ref[:, start : start + step]
            hot = (iota((owners, step), 0) == owner).astype(jnp.float32)
            hot16 = hot.astype(jnp.bfloat16)
            before = jnp.dot(hot16, upper, preferred_element_type=jnp.float32) + carry
            place = jnp.sum(hot * before, axis=0, keepdims=True).astype(jnp.int32)
            carry = carry + jnp.sum(hot, axis=1, keepdims=True)
            target_ref[:, start : start + step] = owner * stride + place
            at_place = (iota((capacity, step), 0) == place).astype(jnp.bfloat16)
            slot = (label // per_cluster).astype(jnp.float32)
            fine = (label % per_cluster).astype(jnp.float32)
            parts = jnp.concatenate([hot * (slot + 1.0), hot * fine], axis=0).astype(jnp.bfloat16)
            table = table + lax.dot_general(
                parts, at_place, (((1,), (1,)), ((), ())), preferred_element_type=jnp.float32
            )
        labels_ref[0] = table[:owners]
        labels_ref[1] = table[owners:]

    return body


def pack_body(capacity, stride, unroll):
    def body(target_ref, rows_ref, labels_ref, packed_ref, source, wide):
        tokens = rows_ref.shape[0]
        total = packed_ref.shape[0]
        wide[...] = jnp.zeros_like(wide)
        for half in range(2):
            owners = labels_ref.shape[1]
            wide[pl.ds(2 * capacity + half, owners, stride=2 * stride), :] = labels_ref[half]
            source[pl.ds(half, tokens, stride=2), :] = rows_ref[
                :, half * LANES : (half + 1) * LANES
            ].astype(jnp.float32)

        def move(index, carry):
            for offset in range(unroll):
                token = index * unroll + offset
                target = target_ref[token]
                wide[pl.ds(2 * target, 2), :] = source[pl.ds(2 * token, 2), :]
            return carry

        lax.fori_loop(0, tokens // unroll, move, 0)
        for half in range(2):
            packed_ref[:, half * LANES : (half + 1) * LANES] = wide[
                pl.ds(half, total, stride=2), :
            ].astype(jnp.bfloat16)

    return body


def sums_body(slots, per_cluster):
    def body(rows_ref, labels_ref, coarse_ref, fine_ref, coarse_out, fine_out, cand_out, norm_out,
             totals, counts):
        columns = slots * per_cluster
        blocks = labels_ref.shape[0]
        group = 4
        totals[...] = jnp.zeros_like(totals)
        counts[...] = jnp.zeros_like(counts)

        def add(index, carry):
            hots = []
            count = counts[...]
            for offset in range(group):
                marks = labels_ref[pl.ds(index * group + offset, 1), :]
                hot = (iota((columns, LANES), 0) == marks).astype(jnp.float32)
                count = count + hot
                hots.append(hot.astype(jnp.bfloat16))
            counts[...] = count
            rows = jnp.concatenate(
                [rows_ref[index * group + offset, :LANES, :] for offset in range(group)], axis=0
            )
            totals[...] += jnp.dot(
                jnp.concatenate(hots, axis=1), rows, preferred_element_type=jnp.float32
            )
            return carry

        lax.fori_loop(0, blocks // group, add, 0)
        for slot in range(slots):
            part = pl.ds(slot * per_cluster, per_cluster)
            sum_f = totals[part, :]
            count_f = jnp.sum(counts[part, :], axis=1, keepdims=True)
            sum_c = jnp.sum(sum_f, axis=0, keepdims=True)
            count_c = jnp.sum(count_f, axis=0, keepdims=True)
            coarse = coarse_ref[slot : slot + 1, :]
            fine = fine_ref[part, :]
            over_c = 1.0 / (count_c + prior_weight)
            over_f = 1.0 / (count_f + prior_weight)
            for step in range(PASSES):
                coarse = (sum_c + prior_weight * coarse) * over_c
                fine = (sum_f - count_f * coarse + prior_weight * fine) * over_f
            coarse_out[slot : slot + 1, :] = coarse
            fine_out[part, :] = fine
            cand = (coarse + fine).astype(jnp.bfloat16)
            value = cand.astype(jnp.float32)
            cand_out[part, :] = (value * -2.0).astype(jnp.bfloat16)
            norm_out[part, :] = jnp.broadcast_to(
                jnp.sum(value * value, axis=1, keepdims=True), (per_cluster, LANES)
            )

    return body


def distance_body(slots, per_cluster):
    def body(rows_ref, labels_ref, cand_ref, norm_ref, out_ref):
        blocks = labels_ref.shape[0]
        pieces = out_ref.shape[0]
        quarter = per_cluster // pieces
        group = 2

        def one(index, carry):
            rows = jnp.concatenate(
                [rows_ref[index * group + offset, :LANES, :] for offset in range(group)], axis=0
            )
            cross = lax.dot_general(
                cand_ref[...], rows, (((1,), (1,)), ((), ())), preferred_element_type=jnp.float32
            )
            for offset in range(group):
                marks = labels_ref[pl.ds(index * group + offset, 1), :]
                held = marks // per_cluster
                value = jnp.zeros((per_cluster, LANES), jnp.float32)
                for slot in range(slots):
                    part = slice(slot * per_cluster, (slot + 1) * per_cluster)
                    term = cross[part, offset * LANES : (offset + 1) * LANES] + norm_ref[part, :]
                    value = jnp.where(held == slot, term, value)
                for piece in range(pieces):
                    out_ref[piece, pl.ds(pl.multiple_of((index * group + offset) * quarter, 8), quarter), :] = value[
                        piece * quarter : (piece + 1) * quarter
                    ]
            return carry

        lax.fori_loop(0, blocks // group, one, 0)

    return body


def pick_body(stride, features):
    def body(got_ref, owner_ref, target_ref, square_ref, out_ref):
        owners, quarter, _ = got_ref.shape
        copies = out_ref.shape[0]
        tokens = owner_ref.shape[1]

        def one(index, carry):
            here = pl.ds(pl.multiple_of(index * LANES, LANES), LANES)
            owner = owner_ref[:, here]
            place = target_ref[:, here] - owner * stride
            place = jnp.broadcast_to(place, (quarter, LANES))
            owner = jnp.broadcast_to(owner, (quarter, LANES))
            value = jnp.zeros((quarter, LANES), jnp.float32)
            for number in range(owners):
                found = jnp.take_along_axis(got_ref[number], place, axis=1)
                value = jnp.where(owner == number, found, value)
            value = (value + square_ref[:, here]) * (1.0 / features)
            for copy in range(copies):
                out_ref[copy, :, here] = value
            return carry

        lax.fori_loop(0, tokens // LANES, one, 0)

    return body


def arrange_body():
    def body(cluster_ref, rows_ref, out_ref):
        def move(index, carry):
            for offset in range(8):
                row = index * 8 + offset
                out_ref[pl.ds(cluster_ref[row], 1), :] = rows_ref[pl.ds(row, 1), :]
            return carry

        lax.fori_loop(0, rows_ref.shape[0] // 8, move, 0)

    return body


def shards(vectors, coarse_init, fine_init, owner_of, slot_in_owner, fine_in_cluster, slot_cluster):
    owners = lax.axis_size("dp")
    pieces = lax.axis_size("grp")
    tokens, width = vectors.shape
    slots, per_cluster, _ = fine_init.shape
    columns = slots * per_cluster
    features = width * pieces
    capacity = 2 * tokens // owners
    stride = capacity + 8
    quarter = per_cluster // pieces
    total = owners * capacity
    f32, bf16, i32 = jnp.float32, jnp.bfloat16, jnp.int32
    shape = jax.ShapeDtypeStruct

    owner = owner_of.reshape(1, tokens)
    label = (slot_in_owner * per_cluster + fine_in_cluster).reshape(1, tokens)
    target, send_labels = call(
        rank_body(owners, capacity, stride, per_cluster),
        (shape((1, tokens), i32), shape((2, owners, capacity), f32)),
        [VMEM] * 2,
        flops=200_000_000,
    )(owner, label)
    send_rows = call(
        pack_body(capacity, stride, 16),
        shape((owners * stride, width), bf16),
        [SMEM, VMEM, VMEM],
        flops=200_000_000,
        scratch=[
            pltpu.VMEM((2 * tokens, LANES), f32),
            pltpu.VMEM((2 * owners * stride, LANES), f32),
        ],
    )(target.reshape(tokens), vectors, send_labels)
    rows = exchanged(send_rows.reshape(owners, stride, width), "dp")
    marks = rows[:, capacity, :].astype(i32)
    labels = (marks[:, :capacity] - 1) * per_cluster + marks[:, capacity:]

    squares = lax.psum(jnp.sum(jnp.square(vectors.astype(f32)), axis=1), "grp").reshape(1, tokens)
    mine = lax.dynamic_slice_in_dim(slot_cluster, lax.axis_index("dp") * slots, slots, 0)
    coarse_mine, fine, cand, norms = call(
        sums_body(slots, per_cluster),
        (
            shape((slots, width), f32),
            shape((columns, width), f32),
            shape((columns, width), bf16),
            shape((columns, LANES), f32),
        ),
        [VMEM] * 4,
        flops=2 * total * columns * width,
        scratch=[pltpu.VMEM((columns, width), f32), pltpu.VMEM((columns, LANES), f32)],
    )(rows, labels, coarse_init[mine], fine_init.reshape(columns, width))

    gathered = exchanged(jnp.broadcast_to(coarse_mine, (owners, slots, width)), "dp")

    partial = call(
        distance_body(slots, per_cluster),
        shape((pieces, owners * quarter, capacity), f32),
        [VMEM] * 4,
        flops=2 * total * columns * width,
    )(rows, labels, cand, norms)
    share = jnp.sum(exchanged(partial, "grp"), axis=0)
    returned = exchanged(share.reshape(owners, quarter, capacity), "dp")
    spread = call(
        pick_body(stride, features),
        shape((pieces, quarter, tokens), f32),
        [VMEM] * 4,
        flops=100_000_000,
    )(returned, owner, target, squares)
    distances = exchanged(spread, "grp").reshape(per_cluster, tokens)
    coarse_out = call(
        arrange_body(),
        shape((owners * slots, width), f32),
        [SMEM, VMEM],
        flops=10_000_000,
    )(slot_cluster, gathered.reshape(owners * slots, width))
    return (coarse_out, fine.reshape(slots, per_cluster, width), distances)


def solution(mesh):
    return jax.shard_map(
        shards,
        mesh=mesh,
        in_specs=(
            P("dp", "grp"),
            P(None, "grp"),
            P("dp", None, "grp"),
            P("dp", None),
            P("dp"),
            P("dp"),
            P(),
        ),
        out_specs=(P(None, "grp"), P("dp", None, "grp"), P(None, "dp")),
        check_vma=False,
    )
```

```python
import jax
import jax.numpy as jnp
from jax import lax
from jax.experimental import pallas as pl
from jax.experimental.pallas import tpu as pltpu
from jax.sharding import PartitionSpec as P

D = 1024
PASSES = 2
LANES = 128


prior_weight = 2.0

VMEM = pl.BlockSpec(memory_space=pltpu.VMEM)
SMEM = pl.BlockSpec(memory_space=pltpu.SMEM)


def call(body, out_shape, ins, flops, scratch=(), mem=16 << 20):
    return pl.pallas_call(
        body,
        out_shape=out_shape,
        in_specs=ins,
        out_specs=jax.tree.map(lambda _: VMEM, out_shape),
        scratch_shapes=list(scratch),
        compiler_params=pltpu.CompilerParams(vmem_limit_bytes=mem),
        cost_estimate=pl.CostEstimate(flops=flops, bytes_accessed=4 << 20, transcendentals=0),
    )


def exchanged(array, axis):
    return lax.all_to_all(array, axis, split_axis=0, concat_axis=0, tiled=True)


def iota(shape, dim):
    return lax.broadcasted_iota(jnp.int32, shape, dim)


def digits(value):
    first = value.astype(jnp.bfloat16).astype(jnp.float32)
    rest = value - first
    second = rest.astype(jnp.bfloat16).astype(jnp.float32)
    return first, second, rest - second


def coded(value):
    top = jnp.max(value, axis=0, keepdims=True)
    power = jnp.ceil(jnp.log2(jnp.maximum(top, 1e-30)))
    code = jnp.minimum(jnp.round(value * jnp.exp2(16.0 - power)), 65535.0) - 32768.0
    return code.astype(jnp.int32).astype(jnp.int16), power


def decoded(code, scale):
    return (code.astype(jnp.int32).astype(jnp.float32) + 32768.0) * scale


def scale_of(power):
    return jnp.exp2(power.astype(jnp.int32).astype(jnp.float32) - 16.0)


def rank_body(owners, capacity, stride, per_cluster):
    def body(owner_ref, label_ref, square_ref, target_ref, meta_ref):
        tokens = owner_ref.shape[1]
        step = 256
        upper = (iota((step, step), 0) < iota((step, step), 1)).astype(jnp.bfloat16)
        carry = jnp.zeros((owners, 1), jnp.float32)
        table = jnp.zeros((5 * owners, capacity), jnp.float32)
        for start in range(0, tokens, step):
            owner = owner_ref[:, start : start + step]
            label = label_ref[:, start : start + step]
            hot = (iota((owners, step), 0) == owner).astype(jnp.float32)
            hot16 = hot.astype(jnp.bfloat16)
            before = jnp.dot(hot16, upper, preferred_element_type=jnp.float32) + carry
            place = jnp.sum(hot * before, axis=0, keepdims=True).astype(jnp.int32)
            carry = carry + jnp.sum(hot, axis=1, keepdims=True)
            target_ref[:, start : start + step] = owner * stride + place
            at_place = (iota((capacity, step), 0) == place).astype(jnp.bfloat16)
            slot = (label // per_cluster).astype(jnp.float32)
            fine = (label % per_cluster).astype(jnp.float32)
            first, second, third = digits(square_ref[:, start : start + step])
            parts = jnp.concatenate(
                [hot * value for value in (slot + 1.0, fine, first, second, third)], axis=0
            ).astype(jnp.bfloat16)
            table = table + lax.dot_general(
                parts, at_place, (((1,), (1,)), ((), ())), preferred_element_type=jnp.float32
            )
        for part in range(5):
            meta_ref[part] = table[part * owners : (part + 1) * owners]

    return body


def pack_body(capacity, stride, unroll):
    def body(target_ref, rows_ref, meta_ref, packed_ref, source, wide):
        tokens = rows_ref.shape[0]
        total = packed_ref.shape[0]
        wide[...] = jnp.zeros_like(wide)
        for part in range(5):
            wide[pl.ds(2 * capacity + part, meta_ref.shape[1], stride=2 * stride), :] = meta_ref[part]
        for half in range(2):
            source[pl.ds(half, tokens, stride=2), :] = rows_ref[
                :, half * LANES : (half + 1) * LANES
            ].astype(jnp.float32)

        def move(index, carry):
            for offset in range(unroll):
                token = index * unroll + offset
                target = target_ref[token]
                wide[pl.ds(2 * target, 2), :] = source[pl.ds(2 * token, 2), :]
            return carry

        lax.fori_loop(0, tokens // unroll, move, 0)
        for half in range(2):
            packed_ref[:, half * LANES : (half + 1) * LANES] = wide[
                pl.ds(half, total, stride=2), :
            ].astype(jnp.bfloat16)

    return body


def sums_body(slots, per_cluster):
    def body(rows_ref, coarse_ref, fine_ref, coarse_out, fine_out, cand_out, norm_out,
             held_out, square_out, totals, counts, labels):
        columns = slots * per_cluster
        blocks, stride, _ = rows_ref.shape
        group = 4
        totals[...] = jnp.zeros_like(totals)
        counts[...] = jnp.zeros_like(counts)

        def read(block, carry):
            meta = rows_ref[block, LANES:stride, :].astype(jnp.float32)
            slot, fine = meta[0:1, :LANES], meta[0:1, LANES:]
            here = pl.ds(block, 1)
            labels[here, :] = ((slot - 1.0) * per_cluster + fine).astype(jnp.int32)
            held_out[here, :] = slot.astype(jnp.int32) - 1
            square_out[here, :] = (meta[1:2, :LANES] + meta[1:2, LANES:]) + meta[2:3, :LANES]
            return carry

        lax.fori_loop(0, blocks, read, 0, unroll=4)

        def add(index, carry):
            hots = []
            count = counts[...]
            for offset in range(group):
                marks = labels[pl.ds(index * group + offset, 1), :]
                hot = (iota((columns, LANES), 0) == marks).astype(jnp.float32)
                count = count + hot
                hots.append(hot.astype(jnp.bfloat16))
            counts[...] = count
            rows = jnp.concatenate(
                [rows_ref[index * group + offset, :LANES, :] for offset in range(group)], axis=0
            )
            totals[...] += jnp.dot(
                jnp.concatenate(hots, axis=1), rows, preferred_element_type=jnp.float32
            )
            return carry

        lax.fori_loop(0, blocks // group, add, 0)
        for slot in range(slots):
            part = pl.ds(slot * per_cluster, per_cluster)
            sum_f = totals[part, :]
            count_f = jnp.sum(counts[part, :], axis=1, keepdims=True)
            sum_c = jnp.sum(sum_f, axis=0, keepdims=True)
            count_c = jnp.sum(count_f, axis=0, keepdims=True)
            coarse = coarse_ref[slot : slot + 1, :]
            fine = fine_ref[part, :]
            over_c = 1.0 / (count_c + prior_weight)
            over_f = 1.0 / (count_f + prior_weight)
            for step in range(PASSES):
                coarse = (sum_c + prior_weight * coarse) * over_c
                fine = (sum_f - count_f * coarse + prior_weight * fine) * over_f
            coarse_out[slot : slot + 1, :] = coarse
            fine_out[part, :] = fine
            cand = (coarse + fine).astype(jnp.bfloat16)
            value = cand.astype(jnp.float32)
            cand_out[part, :] = (value * -2.0).astype(jnp.bfloat16)
            norm_out[part, :] = jnp.broadcast_to(
                jnp.sum(value * value, axis=1, keepdims=True), (per_cluster, LANES)
            )

    return body


def distance_body(slots, per_cluster):
    def body(rows_ref, held_ref, square_ref, cand_ref, norm_ref, out_ref, powers):
        blocks = rows_ref.shape[0]
        pieces = out_ref.shape[0]
        quarter = per_cluster // pieces
        group, pair = 4, 2

        def one(index, carry):
            for first in range(0, group, pair):
                rows = jnp.concatenate(
                    [rows_ref[index * group + first + offset, :LANES, :] for offset in range(pair)],
                    axis=0,
                )
                cross = lax.dot_general(
                    cand_ref[...], rows, (((1,), (1,)), ((), ())),
                    preferred_element_type=jnp.float32,
                )
                for offset in range(pair):
                    block = index * group + first + offset
                    held = held_ref[pl.ds(block, 1), :]
                    value = jnp.zeros((per_cluster, LANES), jnp.float32)
                    for slot in range(slots):
                        part = slice(slot * per_cluster, (slot + 1) * per_cluster)
                        term = cross[part, offset * LANES : (offset + 1) * LANES] + norm_ref[part, :]
                        value = jnp.where(held == slot, term, value)
                    value = jnp.maximum(value + square_ref[pl.ds(block, 1), :], 0.0)
                    code, power = coded(value)
                    powers[pl.ds(block, 1), :] = power
                    for piece in range(pieces):
                        out_ref[piece, pl.ds(pl.multiple_of(block * quarter, quarter), quarter), :] = (
                            code[piece * quarter : (piece + 1) * quarter]
                        )
            return carry

        lax.fori_loop(0, blocks // group, one, 0)
        for piece in range(pieces):
            out_ref[piece, blocks * quarter :, :] = powers[...].astype(jnp.int32).astype(jnp.int16)

    return body


def total_body():
    def body(got_ref, out_ref, scales):
        blocks, quarter, _ = out_ref.shape
        pieces = got_ref.shape[0]
        for piece in range(pieces):
            scales[piece] = scale_of(got_ref[piece, blocks * quarter :, :])

        def one(block, carry):
            here = pl.ds(pl.multiple_of(block * quarter, quarter), quarter)
            value = decoded(got_ref[0, here, :], scales[0, pl.ds(block, 1), :])
            for piece in range(1, pieces):
                value = value + decoded(got_ref[piece, here, :], scales[piece, pl.ds(block, 1), :])
            out_ref[block] = value
            return carry

        lax.fori_loop(0, blocks, one, 0, unroll=4)

    return body


def pick_body(stride, features):
    def body(got_ref, owner_ref, target_ref, out_ref, powers):
        owners, quarter, _ = got_ref.shape
        copies = out_ref.shape[0]
        groups = owner_ref.shape[1] // LANES

        def one(index, carry):
            here = pl.ds(pl.multiple_of(index * LANES, LANES), LANES)
            owner = owner_ref[:, here]
            place = target_ref[:, here] - owner * stride
            place = jnp.broadcast_to(place, (quarter, LANES))
            owner = jnp.broadcast_to(owner, (quarter, LANES))
            value = jnp.zeros((quarter, LANES), jnp.float32)
            for number in range(owners):
                found = jnp.take_along_axis(got_ref[number], place, axis=1)
                value = jnp.where(owner == number, found, value)
            code, power = coded(value * (1.0 / features))
            powers[pl.ds(index, 1), :] = power
            for copy in range(copies):
                out_ref[copy, pl.ds(pl.multiple_of(index * quarter, quarter), quarter), :] = code
            return carry

        lax.fori_loop(0, groups, one, 0)
        for copy in range(copies):
            out_ref[copy, groups * quarter :, :] = powers[...].astype(jnp.int32).astype(jnp.int16)

    return body


def spread_body(quarter):
    def body(got_ref, out_ref):
        groups = out_ref.shape[1] // LANES
        for piece in range(got_ref.shape[0]):
            scales = scale_of(got_ref[piece, groups * quarter :, :])
            for group in range(groups):
                out_ref[piece * quarter : (piece + 1) * quarter, group * LANES : (group + 1) * LANES] = (
                    decoded(
                        got_ref[piece, group * quarter : (group + 1) * quarter, :],
                        scales[group : group + 1],
                    )
                )

    return body


def arrange_body():
    def body(cluster_ref, rows_ref, out_ref):
        def move(index, carry):
            for offset in range(8):
                row = index * 8 + offset
                out_ref[pl.ds(cluster_ref[row], 1), :] = rows_ref[pl.ds(row, 1), :]
            return carry

        lax.fori_loop(0, rows_ref.shape[0] // 8, move, 0)

    return body


def shards(vectors, coarse_init, fine_init, owner_of, slot_in_owner, fine_in_cluster, slot_cluster):
    owners = lax.axis_size("dp")
    pieces = lax.axis_size("grp")
    tokens, width = vectors.shape
    slots, per_cluster, _ = fine_init.shape
    columns = slots * per_cluster
    features = width * pieces
    capacity = 2 * tokens // owners
    stride = capacity + 8
    quarter = per_cluster // pieces
    total = owners * capacity
    f32, bf16, i32 = jnp.float32, jnp.bfloat16, jnp.int32
    shape = jax.ShapeDtypeStruct

    i16 = jnp.int16
    groups = tokens // LANES
    owner = owner_of.reshape(1, tokens)
    label = (slot_in_owner * per_cluster + fine_in_cluster).reshape(1, tokens)
    squares = jnp.sum(jnp.square(vectors.astype(f32)), axis=1).reshape(1, tokens)
    target, meta = call(
        rank_body(owners, capacity, stride, per_cluster),
        (shape((1, tokens), i32), shape((5, owners, capacity), f32)),
        [VMEM] * 3,
        flops=400_000_000,
    )(owner, label, squares)
    send_rows = call(
        pack_body(capacity, stride, 16),
        shape((owners * stride, width), bf16),
        [SMEM, VMEM, VMEM],
        flops=200_000_000,
        scratch=[
            pltpu.VMEM((2 * tokens, LANES), f32),
            pltpu.VMEM((2 * owners * stride, LANES), f32),
        ],
        mem=32 << 20,
    )(target.reshape(tokens), vectors, meta)
    rows = exchanged(send_rows.reshape(owners, stride, width), "dp")
    bits = [bit for bit in (8, 4, 2, 32, 16, 1) if bit < owners]
    masks = [
        sum(bit for place, bit in enumerate(bits) if number >> place & 1) for number in range(owners)
    ]
    order = jnp.bitwise_xor(jnp.array(masks, i32), lax.axis_index("dp"))
    cluster_at = slot_cluster.reshape(owners, slots)[order].reshape(owners * slots)
    mine = lax.dynamic_slice_in_dim(slot_cluster, lax.axis_index("dp") * slots, slots, 0)
    coarse_mine, fine, cand, norms, held, square = call(
        sums_body(slots, per_cluster),
        (
            shape((slots, width), f32),
            shape((columns, width), f32),
            shape((columns, width), bf16),
            shape((columns, LANES), f32),
            shape((owners, LANES), i32),
            shape((owners, LANES), f32),
        ),
        [VMEM] * 3,
        flops=2 * total * columns * width,
        scratch=[
            pltpu.VMEM((columns, width), f32),
            pltpu.VMEM((columns, LANES), f32),
            pltpu.VMEM((owners, LANES), i32),
        ],
        mem=32 << 20,
    )(rows, coarse_init[mine], fine_init.reshape(columns, width))

    with jax.named_scope("centres"):
        gathered = coarse_mine
        for bit in bits:
            other = lax.ppermute(gathered, "dp", [(i, i ^ bit) for i in range(owners)])
            gathered = jnp.concatenate([gathered, other], axis=0)

    with jax.named_scope("measure"):
        partial = call(
            distance_body(slots, per_cluster),
            shape((pieces, owners * quarter + owners, capacity), i16),
            [VMEM] * 5,
            flops=2 * total * columns * width,
            scratch=[pltpu.VMEM((owners, LANES), f32)],
            mem=32 << 20,
        )(rows, held, square, cand, norms)
    share = call(
        total_body(),
        shape((owners, quarter, capacity), f32),
        [VMEM],
        flops=10_000_000,
        scratch=[pltpu.VMEM((pieces, owners, LANES), f32)],
    )(exchanged(partial, "grp"))
    returned = exchanged(share, "dp")
    spread = call(
        pick_body(stride, features),
        shape((pieces, groups * quarter + groups, LANES), i16),
        [VMEM] * 3,
        flops=100_000_000,
        scratch=[pltpu.VMEM((groups, LANES), f32)],
    )(returned, owner, target)
    distances = call(
        spread_body(quarter), shape((per_cluster, tokens), f32), [VMEM], flops=10_000_000
    )(exchanged(spread, "grp"))
    coarse_out = call(
        arrange_body(),
        shape((owners * slots, width), f32),
        [SMEM, VMEM],
        flops=10_000_000,
    )(cluster_at, gathered)
    return (coarse_out, fine.reshape(slots, per_cluster, width), distances)


def solution(mesh):
    return jax.shard_map(
        shards,
        mesh=mesh,
        in_specs=(
            P("dp", "grp"),
            P(None, "grp"),
            P("dp", None, "grp"),
            P("dp", None),
            P("dp"),
            P("dp"),
            P(),
        ),
        out_specs=(P(None, "grp"), P("dp", None, "grp"), P(None, "dp")),
        check_vma=False,
    )
```

```python
import jax
import jax.numpy as jnp
from jax import lax
from jax.experimental import pallas as pl
from jax.experimental.pallas import tpu as pltpu
from jax.sharding import PartitionSpec as P


PASSES = 2
LANES = 128


prior_weight = 2.0

VMEM = pl.BlockSpec(memory_space=pltpu.VMEM)
SMEM = pl.BlockSpec(memory_space=pltpu.SMEM)


def call(body, out_shape, ins, flops, scratch=(), mem=16 << 20):
    return pl.pallas_call(
        body,
        out_shape=out_shape,
        in_specs=ins,
        out_specs=jax.tree.map(lambda _: VMEM, out_shape),
        scratch_shapes=list(scratch),
        compiler_params=pltpu.CompilerParams(vmem_limit_bytes=mem),
        cost_estimate=pl.CostEstimate(flops=flops, bytes_accessed=4 << 20, transcendentals=0),
    )


def exchanged(array, axis):
    return lax.all_to_all(array, axis, split_axis=0, concat_axis=0, tiled=True)


def iota(shape, dim):
    return lax.broadcasted_iota(jnp.int32, shape, dim)


def digits(value):
    first = value.astype(jnp.bfloat16).astype(jnp.float32)
    rest = value - first
    second = rest.astype(jnp.bfloat16).astype(jnp.float32)
    return first, second, rest - second


def coded(value):
    top = jnp.max(value, axis=0, keepdims=True)
    power = jnp.ceil(jnp.log2(jnp.maximum(top, 1e-30)))
    code = jnp.minimum(jnp.round(value * jnp.exp2(16.0 - power)), 65535.0) - 32768.0
    return code.astype(jnp.int32).astype(jnp.int16), power


def decoded(code, scale):
    return (code.astype(jnp.int32).astype(jnp.float32) + 32768.0) * scale


def scale_of(power):
    return jnp.exp2(power.astype(jnp.int32).astype(jnp.float32) - 16.0)


def rank_body(owners, capacity, stride):
    def body(owner_ref, slot_ref, fine_ref, square_ref, target_ref, meta_ref):
        tokens = owner_ref.shape[1]
        step = 256
        upper = (iota((step, step), 0) < iota((step, step), 1)).astype(jnp.bfloat16)
        carry = jnp.zeros((owners, 1), jnp.float32)
        table = jnp.zeros((5 * owners, capacity), jnp.float32)
        for start in range(0, tokens, step):
            owner = owner_ref[:, start : start + step]
            hot = (iota((owners, step), 0) == owner).astype(jnp.float32)
            hot16 = hot.astype(jnp.bfloat16)
            before = jnp.dot(hot16, upper, preferred_element_type=jnp.float32) + carry
            place = jnp.sum(hot * before, axis=0, keepdims=True).astype(jnp.int32)
            carry = carry + jnp.sum(hot, axis=1, keepdims=True)
            target_ref[:, start : start + step] = owner * stride + place
            at_place = (iota((capacity, step), 0) == place).astype(jnp.bfloat16)
            slot = slot_ref[:, start : start + step].astype(jnp.float32)
            fine = fine_ref[:, start : start + step].astype(jnp.float32)
            first, second, third = digits(square_ref[:, start : start + step])
            parts = jnp.concatenate(
                [hot * value for value in (slot + 1.0, fine, first, second, third)], axis=0
            ).astype(jnp.bfloat16)
            table = table + lax.dot_general(
                parts, at_place, (((1,), (1,)), ((), ())), preferred_element_type=jnp.float32
            )
        for part in range(5):
            meta_ref[part] = table[part * owners : (part + 1) * owners]

    return body


def pack_body(capacity, stride, unroll):
    def body(target_ref, rows_ref, meta_ref, packed_ref, source, wide):
        tokens = rows_ref.shape[0]
        total = packed_ref.shape[0]
        wide[...] = jnp.zeros_like(wide)
        for part in range(5):
            wide[pl.ds(2 * capacity + part, meta_ref.shape[1], stride=2 * stride), :] = meta_ref[part]
        for half in range(2):
            source[pl.ds(half, tokens, stride=2), :] = rows_ref[
                :, half * LANES : (half + 1) * LANES
            ].astype(jnp.float32)

        def move(index, carry):
            for offset in range(unroll):
                token = index * unroll + offset
                target = target_ref[token]
                wide[pl.ds(2 * target, 2), :] = source[pl.ds(2 * token, 2), :]
            return carry

        lax.fori_loop(0, tokens // unroll, move, 0)
        for half in range(2):
            packed_ref[:, half * LANES : (half + 1) * LANES] = wide[
                pl.ds(half, total, stride=2), :
            ].astype(jnp.bfloat16)

    return body


def sums_body(slots, per_cluster):
    def body(rows_ref, coarse_ref, fine_ref, coarse_out, fine_out, cand_out, norm_out,
             held_out, square_out, totals, counts, labels):
        columns = slots * per_cluster
        blocks, stride, _ = rows_ref.shape
        group = 16
        totals[...] = jnp.zeros_like(totals)
        counts[...] = jnp.zeros_like(counts)

        def read(block, carry):
            meta = rows_ref[block, LANES:stride, :].astype(jnp.float32)
            slot, fine = meta[0:1, :LANES], meta[0:1, LANES:]
            here = pl.ds(block, 1)
            labels[here, :] = ((slot - 1.0) * per_cluster + fine).astype(jnp.int32)
            held_out[here, :] = slot.astype(jnp.int32) - 1
            square_out[here, :] = (meta[1:2, :LANES] + meta[1:2, LANES:]) + meta[2:3, :LANES]
            return carry

        lax.fori_loop(0, blocks, read, 0, unroll=4)

        ids = iota((columns, LANES), 0).astype(jnp.int16)
        one, zero = jnp.bfloat16(1.0), jnp.bfloat16(0.0)

        def add(index, carry):
            hots = []
            count = jnp.zeros((columns, LANES), jnp.bfloat16)
            for offset in range(group):
                marks = labels[pl.ds(index * group + offset, 1), :]
                hot = jnp.where(ids == marks.astype(jnp.int16), one, zero)
                count = count + hot
                hots.append(hot)
            counts[...] += count.astype(jnp.float32)
            rows = jnp.concatenate(
                [rows_ref[index * group + offset, :LANES, :] for offset in range(group)], axis=0
            )
            totals[...] += jnp.dot(
                jnp.concatenate(hots, axis=1), rows, preferred_element_type=jnp.float32
            )
            return carry

        lax.fori_loop(0, blocks // group, add, 0)
        for slot in range(slots):
            part = pl.ds(slot * per_cluster, per_cluster)
            sum_f = totals[part, :]
            count_f = jnp.sum(counts[part, :], axis=1, keepdims=True)
            sum_c = jnp.sum(sum_f, axis=0, keepdims=True)
            count_c = jnp.sum(count_f, axis=0, keepdims=True)
            coarse = coarse_ref[slot : slot + 1, :]
            fine = fine_ref[part, :]
            over_c = 1.0 / (count_c + prior_weight)
            over_f = 1.0 / (count_f + prior_weight)
            for _ in range(PASSES):
                coarse = (sum_c + prior_weight * coarse) * over_c
                fine = (sum_f - count_f * coarse + prior_weight * fine) * over_f
            coarse_out[slot : slot + 1, :] = coarse
            fine_out[part, :] = fine
            cand = (coarse + fine).astype(jnp.bfloat16)
            value = cand.astype(jnp.float32)
            cand_out[part, :] = (value * -2.0).astype(jnp.bfloat16)
            norm_out[part, :] = jnp.broadcast_to(
                jnp.sum(value * value, axis=1, keepdims=True), (per_cluster, LANES)
            )

    return body


def distance_body(slots, per_cluster):
    def body(rows_ref, held_ref, square_ref, cand_ref, norm_ref, out_ref, powers):
        blocks = rows_ref.shape[0]
        pieces = out_ref.shape[0]
        quarter = per_cluster // pieces
        group, pair = 16, 2

        def one(index, carry):
            for first in range(0, group, pair):
                rows = jnp.concatenate(
                    [rows_ref[index * group + first + offset, :LANES, :] for offset in range(pair)],
                    axis=0,
                )
                cross = lax.dot_general(
                    cand_ref[...], rows, (((1,), (1,)), ((), ())),
                    preferred_element_type=jnp.float32,
                )
                for offset in range(pair):
                    block = index * group + first + offset
                    held = held_ref[pl.ds(block, 1), :]
                    value = jnp.zeros((per_cluster, LANES), jnp.float32)
                    for slot in range(slots):
                        part = slice(slot * per_cluster, (slot + 1) * per_cluster)
                        term = cross[part, offset * LANES : (offset + 1) * LANES] + norm_ref[part, :]
                        value = jnp.where(held == slot, term, value)
                    value = jnp.maximum(value + square_ref[pl.ds(block, 1), :], 0.0)
                    code, power = coded(value)
                    powers[pl.ds(block, 1), :] = power
                    for piece in range(pieces):
                        out_ref[piece, pl.ds(pl.multiple_of(block * quarter, quarter), quarter), :] = (
                            code[piece * quarter : (piece + 1) * quarter]
                        )
            return carry

        lax.fori_loop(0, blocks // group, one, 0)
        for piece in range(pieces):
            out_ref[piece, blocks * quarter :, :] = powers[...].astype(jnp.int32).astype(jnp.int16)

    return body


def total_body():
    def body(got_ref, out_ref, scales):
        blocks, quarter, _ = out_ref.shape
        pieces = got_ref.shape[0]
        for piece in range(pieces):
            scales[piece] = scale_of(got_ref[piece, blocks * quarter :, :])

        def one(block, carry):
            here = pl.ds(pl.multiple_of(block * quarter, quarter), quarter)
            value = decoded(got_ref[0, here, :], scales[0, pl.ds(block, 1), :])
            for piece in range(1, pieces):
                value = value + decoded(got_ref[piece, here, :], scales[piece, pl.ds(block, 1), :])
            out_ref[block] = value
            return carry

        lax.fori_loop(0, blocks, one, 0, unroll=4)

    return body


def pick_body(stride, features):
    def body(got_ref, owner_ref, target_ref, out_ref, powers):
        owners, quarter, _ = got_ref.shape
        copies = out_ref.shape[0]
        groups = owner_ref.shape[1] // LANES

        def one(index, carry):
            here = pl.ds(pl.multiple_of(index * LANES, LANES), LANES)
            owner = owner_ref[:, here]
            place = target_ref[:, here] - owner * stride
            place = jnp.broadcast_to(place, (quarter, LANES))
            owner = jnp.broadcast_to(owner, (quarter, LANES))
            value = jnp.zeros((quarter, LANES), jnp.float32)
            for number in range(owners):
                found = jnp.take_along_axis(got_ref[number], place, axis=1)
                value = jnp.where(owner == number, found, value)
            code, power = coded(value * (1.0 / features))
            powers[pl.ds(index, 1), :] = power
            for copy in range(copies):
                out_ref[copy, pl.ds(pl.multiple_of(index * quarter, quarter), quarter), :] = code
            return carry

        lax.fori_loop(0, groups, one, 0)
        for copy in range(copies):
            out_ref[copy, groups * quarter :, :] = powers[...].astype(jnp.int32).astype(jnp.int16)

    return body


def spread_body(quarter):
    def body(got_ref, out_ref):
        groups = out_ref.shape[1] // LANES
        for piece in range(got_ref.shape[0]):
            scales = scale_of(got_ref[piece, groups * quarter :, :])
            for group in range(groups):
                out_ref[piece * quarter : (piece + 1) * quarter, group * LANES : (group + 1) * LANES] = (
                    decoded(
                        got_ref[piece, group * quarter : (group + 1) * quarter, :],
                        scales[group : group + 1],
                    )
                )

    return body


def arrange_body():
    def body(cluster_ref, rows_ref, out_ref):
        def move(index, carry):
            for offset in range(8):
                row = index * 8 + offset
                out_ref[pl.ds(cluster_ref[row], 1), :] = rows_ref[pl.ds(row, 1), :]
            return carry

        lax.fori_loop(0, rows_ref.shape[0] // 8, move, 0)

    return body


def shards(vectors, coarse_init, fine_init, owner_of, slot_in_owner, fine_in_cluster, slot_cluster):
    owners = lax.axis_size("dp")
    pieces = lax.axis_size("grp")
    tokens, width = vectors.shape
    slots, per_cluster, _ = fine_init.shape
    columns = slots * per_cluster
    features = width * pieces
    capacity = 2 * tokens // owners
    stride = capacity + 8
    quarter = per_cluster // pieces
    total = owners * capacity
    f32, bf16, i32 = jnp.float32, jnp.bfloat16, jnp.int32
    shape = jax.ShapeDtypeStruct

    i16 = jnp.int16
    groups = tokens // LANES
    owner = owner_of.reshape(1, tokens)
    slot, part = slot_in_owner.reshape(1, tokens), fine_in_cluster.reshape(1, tokens)
    squares = jnp.sum(jnp.square(vectors.astype(f32)), axis=1).reshape(1, tokens)
    target, meta = call(
        rank_body(owners, capacity, stride),
        (shape((1, tokens), i32), shape((5, owners, capacity), f32)),
        [VMEM] * 4,
        flops=400_000_000,
    )(owner, slot, part, squares)
    send_rows = call(
        pack_body(capacity, stride, 16),
        shape((owners * stride, width), bf16),
        [SMEM, VMEM, VMEM],
        flops=200_000_000,
        scratch=[
            pltpu.VMEM((2 * tokens, LANES), f32),
            pltpu.VMEM((2 * owners * stride, LANES), f32),
        ],
        mem=32 << 20,
    )(target.reshape(tokens), vectors, meta)
    rows = exchanged(send_rows.reshape(owners, stride, width), "dp")
    bits = [bit for bit in (8, 4, 2, 32, 16, 1) if bit < owners]
    masks = [
        sum(bit for place, bit in enumerate(bits) if number >> place & 1) for number in range(owners)
    ]
    order = jnp.bitwise_xor(jnp.array(masks, i32), lax.axis_index("dp"))
    cluster_at = slot_cluster.reshape(owners, slots)[order].reshape(owners * slots)
    mine = lax.dynamic_slice_in_dim(slot_cluster, lax.axis_index("dp") * slots, slots, 0)
    coarse_mine, fine, cand, norms, held, square = call(
        sums_body(slots, per_cluster),
        (
            shape((slots, width), f32),
            shape((columns, width), f32),
            shape((columns, width), bf16),
            shape((columns, LANES), f32),
            shape((owners, LANES), i32),
            shape((owners, LANES), f32),
        ),
        [VMEM] * 3,
        flops=2 * total * columns * width,
        scratch=[
            pltpu.VMEM((columns, width), f32),
            pltpu.VMEM((columns, LANES), f32),
            pltpu.VMEM((owners, LANES), i32),
        ],
        mem=32 << 20,
    )(rows, coarse_init[mine], fine_init.reshape(columns, width))

    gathered = coarse_mine
    for bit in bits:
        other = lax.ppermute(gathered, "dp", [(i, i ^ bit) for i in range(owners)])
        gathered = jnp.concatenate([gathered, other], axis=0)

    partial = call(
        distance_body(slots, per_cluster),
        shape((pieces, owners * quarter + owners, capacity), i16),
        [VMEM] * 5,
        flops=2 * total * columns * width,
        scratch=[pltpu.VMEM((owners, LANES), f32)],
        mem=32 << 20,
    )(rows, held, square, cand, norms)
    arrived = exchanged(partial, "grp")
    share = call(
        total_body(),
        shape((owners, quarter, capacity), f32),
        [VMEM],
        flops=2_000_000_000,
        scratch=[pltpu.VMEM((pieces, owners, LANES), f32)],
    )(arrived)
    returned = exchanged(share, "dp")
    spread = call(
        pick_body(stride, features),
        shape((pieces, groups * quarter + groups, LANES), i16),
        [VMEM] * 3,
        flops=4_000_000_000,
        scratch=[pltpu.VMEM((groups, LANES), f32)],
    )(returned, owner, target)
    codes = exchanged(spread, "grp")
    coarse_out = call(
        arrange_body(),
        shape((owners * slots, width), f32),
        [SMEM, VMEM],
        flops=2_000_000_000,
    )(cluster_at, gathered)
    distances = call(
        spread_body(quarter), shape((per_cluster, tokens), f32), [VMEM], flops=10_000_000
    )(codes)
    return (coarse_out, fine.reshape(slots, per_cluster, width), distances)


def solution(mesh):
    return jax.shard_map(
        shards,
        mesh=mesh,
        in_specs=(
            P("dp", "grp"),
            P(None, "grp"),
            P("dp", None, "grp"),
            P("dp", None),
            P("dp"),
            P("dp"),
            P(),
        ),
        out_specs=(P(None, "grp"), P("dp", None, "grp"), P(None, "dp")),
        check_vma=False,
    )
```

```python
import jax
import jax.numpy as jnp
from jax import lax
from jax.experimental import pallas as pl
from jax.experimental.pallas import tpu as pltpu
from jax.sharding import PartitionSpec as P


PASSES = 2
LANES = 128
CHUNKS = 4


prior_weight = 2.0

VMEM = pl.BlockSpec(memory_space=pltpu.VMEM)
SMEM = pl.BlockSpec(memory_space=pltpu.SMEM)
HBM = pl.BlockSpec(memory_space=pl.ANY)


def call(body, out_shape, ins, flops, scratch=(), mem=16 << 20, outs=None):
    return pl.pallas_call(
        body,
        out_shape=out_shape,
        in_specs=ins,
        out_specs=outs or jax.tree.map(lambda _: VMEM, out_shape),
        scratch_shapes=list(scratch),
        compiler_params=pltpu.CompilerParams(vmem_limit_bytes=mem),
        cost_estimate=pl.CostEstimate(flops=flops, bytes_accessed=4 << 20, transcendentals=0),
    )


def exchanged(array, axis):
    return lax.all_to_all(array, axis, split_axis=0, concat_axis=0, tiled=True)


def iota(shape, dim):
    return lax.broadcasted_iota(jnp.int32, shape, dim)


def digits(value):
    first = value.astype(jnp.bfloat16).astype(jnp.float32)
    rest = value - first
    second = rest.astype(jnp.bfloat16).astype(jnp.float32)
    return first, second, rest - second


def coded(value):
    top = jnp.max(value, axis=0, keepdims=True)
    power = jnp.ceil(jnp.log2(jnp.maximum(top, 1e-30)))
    code = jnp.minimum(jnp.round(value * jnp.exp2(16.0 - power)), 65535.0) - 32768.0
    return code.astype(jnp.int32).astype(jnp.int16), power


def decoded(code, scale):
    return (code.astype(jnp.int32).astype(jnp.float32) + 32768.0) * scale


def scale_of(power):
    return jnp.exp2(power.astype(jnp.int32).astype(jnp.float32) - 16.0)


def send_body(capacity, stride, chunks, unroll):
    def body(owner_ref, slot_ref, fine_ref, rows_hbm, target_ref, packed_hbm,
             rows, source, wide, packed, targets, done):
        tokens = rows.shape[0]
        total = packed.shape[0]
        owners = total // stride
        step = 256
        load = pltpu.make_async_copy(rows_hbm, rows, done.at[0])
        load.start()
        upper = (iota((step, step), 0) < iota((step, step), 1)).astype(jnp.bfloat16)
        carry = jnp.zeros((owners, 1), jnp.float32)
        for start in range(0, tokens, step):
            owner = owner_ref[:, start : start + step]
            hot = (iota((owners, step), 0) == owner).astype(jnp.float32)
            before = carry + jnp.dot(
                hot.astype(jnp.bfloat16), upper, preferred_element_type=jnp.float32
            )
            place = jnp.sum(hot * before, axis=0, keepdims=True).astype(jnp.int32)
            carry = carry + jnp.sum(hot, axis=1, keepdims=True)
            target_ref[:, start : start + step] = owner * stride + place
        wide[...] = jnp.zeros_like(wide)
        move = pltpu.make_async_copy(target_ref, targets, done.at[1])
        move.start()
        load.wait()
        table = jnp.zeros((5 * owners, capacity), jnp.float32)
        for start in range(0, tokens, step):
            square = jnp.zeros((LANES, step), jnp.float32)
            for half in range(2):
                value = rows[
                    start : start + step, half * LANES : (half + 1) * LANES
                ].astype(jnp.float32)
                source[pl.ds(2 * start + half, step, stride=2), :] = value
                square = square + (value * value).T
            owner = owner_ref[:, start : start + step]
            place = target_ref[:, start : start + step] - owner * stride
            hot = (iota((owners, step), 0) == owner).astype(jnp.float32)
            at_place = (iota((capacity, step), 0) == place).astype(jnp.bfloat16)
            slot = slot_ref[:, start : start + step].astype(jnp.float32)
            fine = fine_ref[:, start : start + step].astype(jnp.float32)
            squares = digits(jnp.sum(square, axis=0, keepdims=True))
            parts = jnp.concatenate(
                [hot * value for value in (slot + 1.0, fine, *squares)], axis=0
            ).astype(jnp.bfloat16)
            table = table + lax.dot_general(
                parts, at_place, (((1,), (1,)), ((), ())), preferred_element_type=jnp.float32
            )
        for part in range(5):
            wide[pl.ds(2 * capacity + part, owners, stride=2 * stride), :] = table[
                part * owners : (part + 1) * owners
            ]
        move.wait()

        def place_rows(index, carry):
            for offset in range(unroll):
                token = index * unroll + offset
                wide[pl.ds(2 * targets[0, token], 2), :] = source[pl.ds(2 * token, 2), :]
            return carry

        lax.fori_loop(0, tokens // unroll, place_rows, 0)
        length = total // chunks
        copies = []
        for chunk in range(chunks):
            part = pl.ds(chunk * length, length)
            for half in range(2):
                packed[part, half * LANES : (half + 1) * LANES] = wide[
                    pl.ds(2 * chunk * length + half, length, stride=2), :
                ].astype(jnp.bfloat16)
            copies.append(
                pltpu.make_async_copy(packed.at[part], packed_hbm.at[part], done.at[2 + chunk])
            )
            if chunk:
                copies[-2].start()
        copies[-1].start()
        for copy in copies:
            copy.wait()

    return body


def fetches(rows_hbm, rows, done, group):
    copies = []
    for chunk in range(rows.shape[0] // group):
        part = pl.ds(chunk * group, group)
        copies.append(pltpu.make_async_copy(rows_hbm.at[part], rows.at[part], done.at[chunk]))
    return copies


def sums_body(slots, per_cluster):
    def body(rows_hbm, coarse_ref, fine_ref, coarse_out, fine_out, cand_out, norm_out,
             held_out, square_out, totals, counts, labels, rows_ref, done):
        columns = slots * per_cluster
        blocks, stride, _ = rows_ref.shape
        group = blocks // CHUNKS
        copies = fetches(rows_hbm, rows_ref, done, group)
        for copy in copies:
            copy.start()
        totals[...] = jnp.zeros_like(totals)
        counts[...] = jnp.zeros_like(counts)

        def read(block, carry):
            meta = rows_ref[block, LANES:stride, :].astype(jnp.float32)
            slot, fine = meta[0:1, :LANES], meta[0:1, LANES:]
            here = pl.ds(block, 1)
            labels[here, :] = ((slot - 1.0) * per_cluster + fine).astype(jnp.int32)
            held_out[here, :] = slot.astype(jnp.int32) - 1
            square_out[here, :] = (meta[1:2, :LANES] + meta[1:2, LANES:]) + meta[2:3, :LANES]
            return carry

        ids = iota((columns, LANES), 0).astype(jnp.int16)
        one, zero = jnp.bfloat16(1.0), jnp.bfloat16(0.0)

        def add(index, carry):
            hots = []
            count = jnp.zeros((columns, LANES), jnp.bfloat16)
            for offset in range(group):
                marks = labels[pl.ds(index * group + offset, 1), :]
                hot = jnp.where(ids == marks.astype(jnp.int16), one, zero)
                count = count + hot
                hots.append(hot)
            counts[...] += count.astype(jnp.float32)
            rows = jnp.concatenate(
                [rows_ref[index * group + offset, :LANES, :] for offset in range(group)], axis=0
            )
            totals[...] += jnp.dot(
                jnp.concatenate(hots, axis=1), rows, preferred_element_type=jnp.float32
            )
            return carry

        for chunk, copy in enumerate(copies):
            copy.wait()
            lax.fori_loop(chunk * group, (chunk + 1) * group, read, 0, unroll=True)
            add(chunk, 0)
        for slot in range(slots):
            part = pl.ds(slot * per_cluster, per_cluster)
            sum_f = totals[part, :]
            count_f = jnp.sum(counts[part, :], axis=1, keepdims=True)
            sum_c = jnp.sum(sum_f, axis=0, keepdims=True)
            count_c = jnp.sum(count_f, axis=0, keepdims=True)
            coarse = coarse_ref[slot : slot + 1, :]
            fine = fine_ref[part, :]
            over_c = 1.0 / (count_c + prior_weight)
            over_f = 1.0 / (count_f + prior_weight)
            for _ in range(PASSES):
                coarse = (sum_c + prior_weight * coarse) * over_c
                fine = (sum_f - count_f * coarse + prior_weight * fine) * over_f
            coarse_out[slot : slot + 1, :] = coarse
            fine_out[part, :] = fine
            cand = (coarse + fine).astype(jnp.bfloat16)
            value = cand.astype(jnp.float32)
            cand_out[part, :] = (value * -2.0).astype(jnp.bfloat16)
            norm_out[part, :] = jnp.broadcast_to(
                jnp.sum(value * value, axis=1, keepdims=True), (per_cluster, LANES)
            )

    return body


def distance_body(slots, per_cluster):
    def body(rows_hbm, held_ref, square_ref, cand_ref, norm_ref, out_ref, powers, rows_ref, done):
        blocks = rows_ref.shape[0]
        pieces = out_ref.shape[0]
        quarter = per_cluster // pieces
        group, pair = blocks // CHUNKS, 2
        copies = fetches(rows_hbm, rows_ref, done, group)
        for copy in copies:
            copy.start()

        def one(index, carry):
            for first in range(0, group, pair):
                rows = jnp.concatenate(
                    [rows_ref[index * group + first + offset, :LANES, :] for offset in range(pair)],
                    axis=0,
                )
                cross = lax.dot_general(
                    cand_ref[...], rows, (((1,), (1,)), ((), ())),
                    preferred_element_type=jnp.float32,
                )
                for offset in range(pair):
                    block = index * group + first + offset
                    held = held_ref[pl.ds(block, 1), :]
                    value = jnp.zeros((per_cluster, LANES), jnp.float32)
                    for slot in range(slots):
                        part = slice(slot * per_cluster, (slot + 1) * per_cluster)
                        term = cross[part, offset * LANES : (offset + 1) * LANES] + norm_ref[part, :]
                        value = jnp.where(held == slot, term, value)
                    value = jnp.maximum(value + square_ref[pl.ds(block, 1), :], 0.0)
                    code, power = coded(value)
                    powers[pl.ds(block, 1), :] = power
                    for piece in range(pieces):
                        out_ref[piece, pl.ds(pl.multiple_of(block * quarter, quarter), quarter), :] = (
                            code[piece * quarter : (piece + 1) * quarter]
                        )
            return carry

        for chunk, copy in enumerate(copies):
            copy.wait()
            one(chunk, 0)
        for piece in range(pieces):
            out_ref[piece, blocks * quarter :, :] = powers[...].astype(jnp.int32).astype(jnp.int16)

    return body


def total_body():
    def body(got_ref, out_ref, scales):
        blocks, quarter, _ = out_ref.shape
        pieces = got_ref.shape[0]
        for piece in range(pieces):
            scales[piece] = scale_of(got_ref[piece, blocks * quarter :, :])

        def one(block, carry):
            here = pl.ds(pl.multiple_of(block * quarter, quarter), quarter)
            value = decoded(got_ref[0, here, :], scales[0, pl.ds(block, 1), :])
            for piece in range(1, pieces):
                value = value + decoded(got_ref[piece, here, :], scales[piece, pl.ds(block, 1), :])
            out_ref[block] = value
            return carry

        lax.fori_loop(0, blocks, one, 0, unroll=4)

    return body


def pick_body(stride, features):
    def body(got_ref, owner_ref, target_ref, out_ref, powers):
        owners, quarter, _ = got_ref.shape
        copies = out_ref.shape[0]
        groups = owner_ref.shape[1] // LANES

        def one(index, carry):
            here = pl.ds(pl.multiple_of(index * LANES, LANES), LANES)
            owner = owner_ref[:, here]
            place = target_ref[:, here] - owner * stride
            place = jnp.broadcast_to(place, (quarter, LANES))
            owner = jnp.broadcast_to(owner, (quarter, LANES))
            value = jnp.zeros((quarter, LANES), jnp.float32)
            for number in range(owners):
                found = jnp.take_along_axis(got_ref[number], place, axis=1, mode="promise_in_bounds")
                value = jnp.where(owner == number, found, value)
            code, power = coded(value * (1.0 / features))
            powers[pl.ds(index, 1), :] = power
            for copy in range(copies):
                out_ref[copy, pl.ds(pl.multiple_of(index * quarter, quarter), quarter), :] = code
            return carry

        lax.fori_loop(0, groups, one, 0, unroll=2)
        for copy in range(copies):
            out_ref[copy, groups * quarter :, :] = powers[...].astype(jnp.int32).astype(jnp.int16)

    return body


def spread_body(quarter):
    def body(got_ref, out_ref):
        groups = out_ref.shape[1] // LANES
        for piece in range(got_ref.shape[0]):
            scales = scale_of(got_ref[piece, groups * quarter :, :])
            for group in range(groups):
                out_ref[piece * quarter : (piece + 1) * quarter, group * LANES : (group + 1) * LANES] = (
                    decoded(
                        got_ref[piece, group * quarter : (group + 1) * quarter, :],
                        scales[group : group + 1],
                    )
                )

    return body


def arrange_body():
    def body(cluster_ref, rows_ref, out_ref):
        def move(index, carry):
            for offset in range(8):
                row = index * 8 + offset
                out_ref[pl.ds(cluster_ref[row], 1), :] = rows_ref[pl.ds(row, 1), :]
            return carry

        lax.fori_loop(0, rows_ref.shape[0] // 8, move, 0)

    return body


def shards(vectors, coarse_init, fine_init, owner_of, slot_in_owner, fine_in_cluster, slot_cluster):
    owners = lax.axis_size("dp")
    pieces = lax.axis_size("grp")
    tokens, width = vectors.shape
    slots, per_cluster, _ = fine_init.shape
    columns = slots * per_cluster
    features = width * pieces
    capacity = 2 * tokens // owners
    stride = capacity + 8
    quarter = per_cluster // pieces
    total = owners * capacity
    f32, bf16, i32 = jnp.float32, jnp.bfloat16, jnp.int32
    shape = jax.ShapeDtypeStruct

    i16 = jnp.int16
    groups = tokens // LANES
    owner = owner_of.reshape(1, tokens)
    slot, part = slot_in_owner.reshape(1, tokens), fine_in_cluster.reshape(1, tokens)
    target, send_rows = call(
        send_body(capacity, stride, 4, 32),
        (shape((1, tokens), i32), shape((owners * stride, width), bf16)),
        [VMEM, VMEM, VMEM, HBM],
        flops=400_000_000,
        scratch=[
            pltpu.VMEM((tokens, width), bf16),
            pltpu.VMEM((2 * tokens, LANES), f32),
            pltpu.VMEM((2 * owners * stride, LANES), f32),
            pltpu.VMEM((owners * stride, width), bf16),
            pltpu.SMEM((1, tokens), i32),
            pltpu.SemaphoreType.DMA((6,)),
        ],
        mem=56 << 20,
        outs=(VMEM, HBM),
    )(owner, slot, part, vectors)
    rows = exchanged(send_rows.reshape(owners, stride, width), "dp")
    bits = [bit for bit in (8, 4, 2, 32, 16, 1) if bit < owners]
    masks = [
        sum(bit for place, bit in enumerate(bits) if number >> place & 1) for number in range(owners)
    ]
    order = jnp.bitwise_xor(jnp.array(masks, i32), lax.axis_index("dp"))
    cluster_at = slot_cluster.reshape(owners, slots)[order].reshape(owners * slots)
    mine = lax.dynamic_slice_in_dim(slot_cluster, lax.axis_index("dp") * slots, slots, 0)
    coarse_mine, fine, cand, norms, held, square = call(
        sums_body(slots, per_cluster),
        (
            shape((slots, width), f32),
            shape((columns, width), f32),
            shape((columns, width), bf16),
            shape((columns, LANES), f32),
            shape((owners, LANES), i32),
            shape((owners, LANES), f32),
        ),
        [HBM, VMEM, VMEM],
        flops=2 * total * columns * width,
        scratch=[
            pltpu.VMEM((columns, width), f32),
            pltpu.VMEM((columns, LANES), f32),
            pltpu.VMEM((owners, LANES), i32),
            pltpu.VMEM((owners, stride, width), bf16),
            pltpu.SemaphoreType.DMA((CHUNKS,)),
        ],
        mem=32 << 20,
    )(rows, coarse_init[mine], fine_init.reshape(columns, width))

    gathered = coarse_mine
    for bit in bits:
        other = lax.ppermute(gathered, "dp", [(i, i ^ bit) for i in range(owners)])
        gathered = jnp.concatenate([gathered, other], axis=0)

    partial = call(
        distance_body(slots, per_cluster),
        shape((pieces, owners * quarter + owners, capacity), i16),
        [HBM, VMEM, VMEM, VMEM, VMEM],
        flops=2 * total * columns * width,
        scratch=[
            pltpu.VMEM((owners, LANES), f32),
            pltpu.VMEM((owners, stride, width), bf16),
            pltpu.SemaphoreType.DMA((CHUNKS,)),
        ],
        mem=32 << 20,
    )(rows, held, square, cand, norms)
    arrived = exchanged(partial, "grp")
    share = call(
        total_body(),
        shape((owners, quarter, capacity), f32),
        [VMEM],
        flops=2_000_000_000,
        scratch=[pltpu.VMEM((pieces, owners, LANES), f32)],
    )(arrived)
    returned = exchanged(share, "dp")
    spread = call(
        pick_body(stride, features),
        shape((pieces, groups * quarter + groups, LANES), i16),
        [VMEM] * 3,
        flops=4_000_000_000,
        scratch=[pltpu.VMEM((groups, LANES), f32)],
    )(returned, owner, target)
    codes = exchanged(spread, "grp")
    coarse_out = call(
        arrange_body(),
        shape((owners * slots, width), f32),
        [SMEM, VMEM],
        flops=2_000_000_000,
    )(cluster_at, gathered)
    distances = call(
        spread_body(quarter), shape((per_cluster, tokens), f32), [VMEM], flops=10_000_000
    )(codes)
    return (coarse_out, fine.reshape(slots, per_cluster, width), distances)


def solution(mesh):
    return jax.shard_map(
        shards,
        mesh=mesh,
        in_specs=(
            P("dp", "grp"),
            P(None, "grp"),
            P("dp", None, "grp"),
            P("dp", None),
            P("dp"),
            P("dp"),
            P(),
        ),
        out_specs=(P(None, "grp"), P("dp", None, "grp"), P(None, "dp")),
        check_vma=False,
    )
```

```python
import jax
import jax.numpy as jnp
from jax import lax
from jax.experimental import pallas as pl
from jax.experimental.pallas import tpu as pltpu
from jax.sharding import PartitionSpec as P


PASSES = 2
LANES = 128
CHUNKS = 4


prior_weight = 2.0

VMEM = pl.BlockSpec(memory_space=pltpu.VMEM)
SMEM = pl.BlockSpec(memory_space=pltpu.SMEM)
HBM = pl.BlockSpec(memory_space=pl.ANY)


def call(body, out_shape, ins, flops, scratch=(), mem=16 << 20, outs=None):
    return pl.pallas_call(
        body,
        out_shape=out_shape,
        in_specs=ins,
        out_specs=outs or jax.tree.map(lambda _: VMEM, out_shape),
        scratch_shapes=list(scratch),
        compiler_params=pltpu.CompilerParams(vmem_limit_bytes=mem),
        cost_estimate=pl.CostEstimate(flops=flops, bytes_accessed=4 << 20, transcendentals=0),
    )


def exchanged(array, axis):
    return lax.all_to_all(array, axis, split_axis=0, concat_axis=0, tiled=True)


def iota(shape, dim):
    return lax.broadcasted_iota(jnp.int32, shape, dim)


def digits(value):
    first = value.astype(jnp.bfloat16).astype(jnp.float32)
    rest = value - first
    second = rest.astype(jnp.bfloat16).astype(jnp.float32)
    return first, second, rest - second


def coded(value):
    top = jnp.max(value, axis=0, keepdims=True)
    power = jnp.ceil(jnp.log2(jnp.maximum(top, 1e-30)))
    code = jnp.minimum(jnp.round(value * jnp.exp2(16.0 - power)), 65535.0) - 32768.0
    return code.astype(jnp.int32).astype(jnp.int16), power


def decoded(code, scale):
    return (code.astype(jnp.int32).astype(jnp.float32) + 32768.0) * scale


def scale_of(power):
    return jnp.exp2(power.astype(jnp.int32).astype(jnp.float32) - 16.0)


def floated(value):
    power = jnp.floor(jnp.log2(jnp.maximum(value, 2.0**-21)))
    power = jnp.clip(power, -21.0, 9.0)
    code = 2048.0 * (power + 21.0) + jnp.round(value * jnp.exp2(-power) * 2048.0)
    code = jnp.minimum(code, 65535.0).astype(jnp.int32)
    half = value.shape[0] // 2
    return code[:half] | (code[half:] << 16)


def unfloated(code):
    octave = jnp.maximum((code >> 11) - 1, 0)
    mantissa = (code - (octave << 11)).astype(jnp.float32)
    return mantissa * jnp.exp2(octave.astype(jnp.float32) - 32.0)


def send_body(capacity, stride, chunks, unroll):
    def body(owner_ref, slot_ref, fine_ref, rows_hbm, target_ref, packed_hbm,
             rows, source, wide, packed, targets, done):
        tokens = rows.shape[0]
        total = packed.shape[0]
        owners = total // stride
        step = 256
        load = pltpu.make_async_copy(rows_hbm, rows, done.at[0])
        load.start()
        upper = (iota((step, step), 0) < iota((step, step), 1)).astype(jnp.bfloat16)
        carry = jnp.zeros((owners, 1), jnp.float32)
        for start in range(0, tokens, step):
            owner = owner_ref[:, start : start + step]
            hot = (iota((owners, step), 0) == owner).astype(jnp.float32)
            before = carry + jnp.dot(
                hot.astype(jnp.bfloat16), upper, preferred_element_type=jnp.float32
            )
            place = jnp.sum(hot * before, axis=0, keepdims=True).astype(jnp.int32)
            carry = carry + jnp.sum(hot, axis=1, keepdims=True)
            target_ref[:, start : start + step] = owner * stride + place
        wide[...] = jnp.zeros_like(wide)
        move = pltpu.make_async_copy(target_ref, targets, done.at[1])
        move.start()
        load.wait()
        table = jnp.zeros((5 * owners, capacity), jnp.float32)
        for start in range(0, tokens, step):
            square = jnp.zeros((LANES, step), jnp.float32)
            for half in range(2):
                value = rows[
                    start : start + step, half * LANES : (half + 1) * LANES
                ].astype(jnp.float32)
                source[pl.ds(2 * start + half, step, stride=2), :] = value
                square = square + (value * value).T
            owner = owner_ref[:, start : start + step]
            place = target_ref[:, start : start + step] - owner * stride
            hot = (iota((owners, step), 0) == owner).astype(jnp.float32)
            at_place = (iota((capacity, step), 0) == place).astype(jnp.bfloat16)
            slot = slot_ref[:, start : start + step].astype(jnp.float32)
            fine = fine_ref[:, start : start + step].astype(jnp.float32)
            squares = digits(jnp.sum(square, axis=0, keepdims=True))
            parts = jnp.concatenate(
                [hot * value for value in (slot + 1.0, fine, *squares)], axis=0
            ).astype(jnp.bfloat16)
            table = table + lax.dot_general(
                parts, at_place, (((1,), (1,)), ((), ())), preferred_element_type=jnp.float32
            )
        for part in range(5):
            wide[pl.ds(2 * capacity + part, owners, stride=2 * stride), :] = table[
                part * owners : (part + 1) * owners
            ]
        move.wait()

        def place_rows(index, carry):
            for offset in range(unroll):
                token = index * unroll + offset
                wide[pl.ds(2 * targets[0, token], 2), :] = source[pl.ds(2 * token, 2), :]
            return carry

        lax.fori_loop(0, tokens // unroll, place_rows, 0)
        length = total // chunks
        copies = []
        for chunk in range(chunks):
            part = pl.ds(chunk * length, length)
            for half in range(2):
                packed[part, half * LANES : (half + 1) * LANES] = wide[
                    pl.ds(2 * chunk * length + half, length, stride=2), :
                ].astype(jnp.bfloat16)
            copies.append(
                pltpu.make_async_copy(packed.at[part], packed_hbm.at[part], done.at[2 + chunk])
            )
            if chunk:
                copies[-2].start()
        copies[-1].start()
        for copy in copies:
            copy.wait()

    return body


def fetches(rows_hbm, rows, done, group):
    copies = []
    for chunk in range(rows.shape[0] // group):
        part = pl.ds(chunk * group, group)
        copies.append(pltpu.make_async_copy(rows_hbm.at[part], rows.at[part], done.at[chunk]))
    return copies


def sums_body(slots, per_cluster):
    def body(rows_ref, coarse_ref, fine_ref, coarse_out, fine_out, cand_out, norm_out,
             held_out, square_out, totals, counts, labels):
        columns = slots * per_cluster
        blocks, stride, _ = rows_ref.shape
        group = 16
        totals[...] = jnp.zeros_like(totals)
        counts[...] = jnp.zeros_like(counts)

        def read(block, carry):
            meta = rows_ref[block, LANES:stride, :].astype(jnp.float32)
            slot, fine = meta[0:1, :LANES], meta[0:1, LANES:]
            here = pl.ds(block, 1)
            labels[here, :] = ((slot - 1.0) * per_cluster + fine).astype(jnp.int32)
            held_out[here, :] = slot.astype(jnp.int32) - 1
            square_out[here, :] = (meta[1:2, :LANES] + meta[1:2, LANES:]) + meta[2:3, :LANES]
            return carry

        lax.fori_loop(0, blocks, read, 0, unroll=4)

        ids = iota((columns, LANES), 0).astype(jnp.int16)
        one, zero = jnp.bfloat16(1.0), jnp.bfloat16(0.0)

        def add(index, carry):
            hots = []
            count = jnp.zeros((columns, LANES), jnp.bfloat16)
            for offset in range(group):
                marks = labels[pl.ds(index * group + offset, 1), :]
                hot = jnp.where(ids == marks.astype(jnp.int16), one, zero)
                count = count + hot
                hots.append(hot)
            counts[...] += count.astype(jnp.float32)
            rows = jnp.concatenate(
                [rows_ref[index * group + offset, :LANES, :] for offset in range(group)], axis=0
            )
            totals[...] += jnp.dot(
                jnp.concatenate(hots, axis=1), rows, preferred_element_type=jnp.float32
            )
            return carry

        lax.fori_loop(0, blocks // group, add, 0)
        for slot in range(slots):
            part = pl.ds(slot * per_cluster, per_cluster)
            sum_f = totals[part, :]
            count_f = jnp.sum(counts[part, :], axis=1, keepdims=True)
            sum_c = jnp.sum(sum_f, axis=0, keepdims=True)
            count_c = jnp.sum(count_f, axis=0, keepdims=True)
            coarse = coarse_ref[slot : slot + 1, :]
            fine = fine_ref[part, :]
            over_c = 1.0 / (count_c + prior_weight)
            over_f = 1.0 / (count_f + prior_weight)
            for _ in range(PASSES):
                coarse = (sum_c + prior_weight * coarse) * over_c
                fine = (sum_f - count_f * coarse + prior_weight * fine) * over_f
            coarse_out[slot : slot + 1, :] = coarse
            fine_out[part, :] = fine
            cand = (coarse + fine).astype(jnp.bfloat16)
            value = cand.astype(jnp.float32)
            cand_out[part, :] = (value * -2.0).astype(jnp.bfloat16)
            norm_out[part, :] = jnp.broadcast_to(
                jnp.sum(value * value, axis=1, keepdims=True), (per_cluster, LANES)
            )

    return body


def distance_body(slots, per_cluster):
    def body(rows_hbm, held_ref, square_ref, cand_ref, norm_ref, out_ref, powers, rows_ref, done):
        blocks = rows_ref.shape[0]
        pieces = out_ref.shape[0]
        quarter = per_cluster // pieces
        group, pair = blocks // CHUNKS, 2
        copies = fetches(rows_hbm, rows_ref, done, group)
        for copy in copies:
            copy.start()

        def one(index, carry):
            for first in range(0, group, pair):
                rows = jnp.concatenate(
                    [rows_ref[index * group + first + offset, :LANES, :] for offset in range(pair)],
                    axis=0,
                )
                cross = lax.dot_general(
                    cand_ref[...], rows, (((1,), (1,)), ((), ())),
                    preferred_element_type=jnp.float32,
                )
                for offset in range(pair):
                    block = index * group + first + offset
                    held = held_ref[pl.ds(block, 1), :]
                    value = jnp.zeros((per_cluster, LANES), jnp.float32)
                    for slot in range(slots):
                        part = slice(slot * per_cluster, (slot + 1) * per_cluster)
                        term = cross[part, offset * LANES : (offset + 1) * LANES] + norm_ref[part, :]
                        value = jnp.where(held == slot, term, value)
                    value = jnp.maximum(value + square_ref[pl.ds(block, 1), :], 0.0)
                    code, power = coded(value)
                    powers[pl.ds(block, 1), :] = power
                    for piece in range(pieces):
                        out_ref[piece, pl.ds(pl.multiple_of(block * quarter, quarter), quarter), :] = (
                            code[piece * quarter : (piece + 1) * quarter]
                        )
            return carry

        for chunk, copy in enumerate(copies):
            copy.wait()
            one(chunk, 0)
        for piece in range(pieces):
            out_ref[piece, blocks * quarter :, :] = powers[...].astype(jnp.int32).astype(jnp.int16)

    return body


def total_body(features):
    def body(got_ref, out_ref, scales):
        blocks, half, _ = out_ref.shape
        pieces = got_ref.shape[0]
        quarter = 2 * half
        for piece in range(pieces):
            scales[piece] = scale_of(got_ref[piece, blocks * quarter :, :])

        def one(block, carry):
            here = pl.ds(pl.multiple_of(block * quarter, quarter), quarter)
            value = decoded(got_ref[0, here, :], scales[0, pl.ds(block, 1), :])
            for piece in range(1, pieces):
                value = value + decoded(got_ref[piece, here, :], scales[piece, pl.ds(block, 1), :])
            out_ref[block] = floated(value * (1.0 / features))
            return carry

        lax.fori_loop(0, blocks, one, 0, unroll=8)

    return body


def pick_body(stride):
    def body(got_ref, owner_ref, target_ref, out_ref):
        owners, half, _ = got_ref.shape
        copies = out_ref.shape[0]
        groups = owner_ref.shape[1] // LANES

        def one(index, carry):
            here = pl.ds(pl.multiple_of(index * LANES, LANES), LANES)
            owner = owner_ref[:, here]
            place = target_ref[:, here] - owner * stride
            place = jnp.broadcast_to(place, (half, LANES))
            owner = jnp.broadcast_to(owner, (half, LANES))
            value = jnp.zeros((half, LANES), jnp.int32)
            for number in range(owners):
                found = jnp.take_along_axis(
                    got_ref[number], place, axis=1, mode="promise_in_bounds"
                )
                value = jnp.where(owner == number, found, value)
            for copy in range(copies):
                out_ref[copy, :, here] = value
            return carry

        lax.fori_loop(0, groups, one, 0, unroll=4)

    return body


def spread_body():
    def body(got_ref, out_ref):
        pieces, half, _ = got_ref.shape
        for piece in range(pieces):
            code = got_ref[piece]
            for part, value in enumerate((code & 65535, lax.shift_right_logical(code, 16))):
                start = (2 * piece + part) * half
                out_ref[start : start + half, :] = unfloated(value)

    return body


def arrange_body():
    def body(cluster_ref, rows_ref, out_ref):
        def move(index, carry):
            for offset in range(8):
                row = index * 8 + offset
                out_ref[pl.ds(cluster_ref[row], 1), :] = rows_ref[pl.ds(row, 1), :]
            return carry

        lax.fori_loop(0, rows_ref.shape[0] // 8, move, 0)

    return body


def shards(vectors, coarse_init, fine_init, owner_of, slot_in_owner, fine_in_cluster, slot_cluster):
    owners = lax.axis_size("dp")
    pieces = lax.axis_size("grp")
    tokens, width = vectors.shape
    slots, per_cluster, _ = fine_init.shape
    columns = slots * per_cluster
    features = width * pieces
    capacity = 2 * tokens // owners
    stride = capacity + 8
    quarter = per_cluster // pieces
    total = owners * capacity
    f32, bf16, i32 = jnp.float32, jnp.bfloat16, jnp.int32
    shape = jax.ShapeDtypeStruct

    i16 = jnp.int16
    owner = owner_of.reshape(1, tokens)
    slot, part = slot_in_owner.reshape(1, tokens), fine_in_cluster.reshape(1, tokens)
    target, send_rows = call(
        send_body(capacity, stride, 4, 32),
        (shape((1, tokens), i32), shape((owners * stride, width), bf16)),
        [VMEM, VMEM, VMEM, HBM],
        flops=400_000_000,
        scratch=[
            pltpu.VMEM((tokens, width), bf16),
            pltpu.VMEM((2 * tokens, LANES), f32),
            pltpu.VMEM((2 * owners * stride, LANES), f32),
            pltpu.VMEM((owners * stride, width), bf16),
            pltpu.SMEM((1, tokens), i32),
            pltpu.SemaphoreType.DMA((6,)),
        ],
        mem=56 << 20,
        outs=(VMEM, HBM),
    )(owner, slot, part, vectors)
    rows = exchanged(send_rows.reshape(owners, stride, width), "dp")
    bits = [bit for bit in (8, 4, 2, 32, 16, 1) if bit < owners]
    masks = [
        sum(bit for place, bit in enumerate(bits) if number >> place & 1) for number in range(owners)
    ]
    order = jnp.bitwise_xor(jnp.array(masks, i32), lax.axis_index("dp"))
    cluster_at = slot_cluster.reshape(owners, slots)[order].reshape(owners * slots)
    mine = lax.dynamic_slice_in_dim(slot_cluster, lax.axis_index("dp") * slots, slots, 0)
    coarse_mine, fine, cand, norms, held, square = call(
        sums_body(slots, per_cluster),
        (
            shape((slots, width), f32),
            shape((columns, width), f32),
            shape((columns, width), bf16),
            shape((columns, LANES), f32),
            shape((owners, LANES), i32),
            shape((owners, LANES), f32),
        ),
        [VMEM] * 3,
        flops=2 * total * columns * width,
        scratch=[
            pltpu.VMEM((columns, width), f32),
            pltpu.VMEM((columns, LANES), f32),
            pltpu.VMEM((owners, LANES), i32),
        ],
        mem=32 << 20,
    )(rows, coarse_init[mine], fine_init.reshape(columns, width))

    gathered = coarse_mine
    for bit in bits:
        other = lax.ppermute(gathered, "dp", [(i, i ^ bit) for i in range(owners)])
        gathered = jnp.concatenate([gathered, other], axis=0)

    partial = call(
        distance_body(slots, per_cluster),
        shape((pieces, owners * quarter + owners, capacity), i16),
        [HBM, VMEM, VMEM, VMEM, VMEM],
        flops=2 * total * columns * width,
        scratch=[
            pltpu.VMEM((owners, LANES), f32),
            pltpu.VMEM((owners, stride, width), bf16),
            pltpu.SemaphoreType.DMA((CHUNKS,)),
        ],
        mem=32 << 20,
    )(rows, held, square, cand, norms)
    arrived = exchanged(partial, "grp")
    share = call(
        total_body(features),
        shape((owners, quarter // 2, capacity), i32),
        [VMEM],
        flops=2_000_000_000,
        scratch=[pltpu.VMEM((pieces, owners, LANES), f32)],
    )(arrived)
    returned = exchanged(share, "dp")
    spread = call(
        pick_body(stride),
        shape((pieces, quarter // 2, tokens), i32),
        [VMEM] * 3,
        flops=4_000_000_000,
    )(returned, owner, target)
    codes = exchanged(spread, "grp")
    coarse_out = call(
        arrange_body(),
        shape((owners * slots, width), f32),
        [SMEM, VMEM],
        flops=2_000_000_000,
    )(cluster_at, gathered)
    distances = call(
        spread_body(), shape((per_cluster, tokens), f32), [VMEM], flops=10_000_000
    )(codes)
    return (coarse_out, fine.reshape(slots, per_cluster, width), distances)


def solution(mesh):
    return jax.shard_map(
        shards,
        mesh=mesh,
        in_specs=(
            P("dp", "grp"),
            P(None, "grp"),
            P("dp", None, "grp"),
            P("dp", None),
            P("dp"),
            P("dp"),
            P(),
        ),
        out_specs=(P(None, "grp"), P("dp", None, "grp"), P(None, "dp")),
        check_vma=False,
    )
```

```python
import jax
import jax.numpy as jnp
from jax import lax
from jax.experimental import pallas as pl
from jax.experimental.pallas import tpu as pltpu
from jax.sharding import PartitionSpec as P


PASSES = 2
LANES = 128
CHUNKS = 4


prior_weight = 2.0

VMEM = pl.BlockSpec(memory_space=pltpu.VMEM)
SMEM = pl.BlockSpec(memory_space=pltpu.SMEM)
HBM = pl.BlockSpec(memory_space=pl.ANY)


def call(body, out_shape, ins, flops, scratch=(), mem=16 << 20, outs=None):
    return pl.pallas_call(
        body,
        out_shape=out_shape,
        in_specs=ins,
        out_specs=outs or jax.tree.map(lambda _: VMEM, out_shape),
        scratch_shapes=list(scratch),
        compiler_params=pltpu.CompilerParams(vmem_limit_bytes=mem),
        cost_estimate=pl.CostEstimate(flops=flops, bytes_accessed=4 << 20, transcendentals=0),
    )


def exchanged(array, axis):
    return lax.all_to_all(array, axis, split_axis=0, concat_axis=0, tiled=True)


def iota(shape, dim):
    return lax.broadcasted_iota(jnp.int32, shape, dim)


def digits(value):
    first = value.astype(jnp.bfloat16).astype(jnp.float32)
    rest = value - first
    second = rest.astype(jnp.bfloat16).astype(jnp.float32)
    return first, second, rest - second


def coded(value):
    top = jnp.max(value, axis=0, keepdims=True)
    power = jnp.ceil(jnp.log2(jnp.maximum(top, 1e-30)))
    code = jnp.minimum(jnp.round(value * jnp.exp2(16.0 - power)), 65535.0) - 32768.0
    return code.astype(jnp.int32).astype(jnp.int16), power


def decoded(code, scale):
    return (code.astype(jnp.int32).astype(jnp.float32) + 32768.0) * scale


def scale_of(power):
    return jnp.exp2(power.astype(jnp.int32).astype(jnp.float32) - 16.0)


def floated(value):
    power = jnp.floor(jnp.log2(jnp.maximum(value, 2.0**-21)))
    power = jnp.clip(power, -21.0, 9.0)
    code = 2048.0 * (power + 21.0) + jnp.round(value * jnp.exp2(-power) * 2048.0)
    code = jnp.minimum(code, 65535.0).astype(jnp.int32)
    half = value.shape[0] // 2
    return code[:half] | (code[half:] << 16)


def unfloated(code):
    octave = jnp.maximum((code >> 11) - 1, 0)
    mantissa = (code - (octave << 11)).astype(jnp.float32)
    return mantissa * jnp.exp2(octave.astype(jnp.float32) - 32.0)


def send_body(capacity, stride, chunks, unroll):
    def body(owner_ref, slot_ref, fine_ref, rows_hbm, target_ref, packed_hbm,
             rows, source, wide, packed, targets, done):
        tokens = rows.shape[0]
        total = packed.shape[0]
        owners = total // stride
        step = 256
        load = pltpu.make_async_copy(rows_hbm, rows, done.at[0])
        load.start()
        upper = (iota((step, step), 0) < iota((step, step), 1)).astype(jnp.bfloat16)
        carry = jnp.zeros((owners, 1), jnp.float32)
        for start in range(0, tokens, step):
            owner = owner_ref[:, start : start + step]
            hot = (iota((owners, step), 0) == owner).astype(jnp.float32)
            before = carry + jnp.dot(
                hot.astype(jnp.bfloat16), upper, preferred_element_type=jnp.float32
            )
            place = jnp.sum(hot * before, axis=0, keepdims=True).astype(jnp.int32)
            carry = carry + jnp.sum(hot, axis=1, keepdims=True)
            target_ref[:, start : start + step] = owner * stride + place
        wide[...] = jnp.zeros_like(wide)
        move = pltpu.make_async_copy(target_ref, targets, done.at[1])
        move.start()
        load.wait()
        table = jnp.zeros((5 * owners, capacity), jnp.float32)
        for start in range(0, tokens, step):
            square = jnp.zeros((LANES, step), jnp.float32)
            for half in range(2):
                value = rows[
                    start : start + step, half * LANES : (half + 1) * LANES
                ].astype(jnp.float32)
                source[pl.ds(2 * start + half, step, stride=2), :] = value
                square = square + (value * value).T
            owner = owner_ref[:, start : start + step]
            place = target_ref[:, start : start + step] - owner * stride
            hot = (iota((owners, step), 0) == owner).astype(jnp.float32)
            at_place = (iota((capacity, step), 0) == place).astype(jnp.bfloat16)
            slot = slot_ref[:, start : start + step].astype(jnp.float32)
            fine = fine_ref[:, start : start + step].astype(jnp.float32)
            squares = digits(jnp.sum(square, axis=0, keepdims=True))
            parts = jnp.concatenate(
                [hot * value for value in (slot + 1.0, fine, *squares)], axis=0
            ).astype(jnp.bfloat16)
            table = table + lax.dot_general(
                parts, at_place, (((1,), (1,)), ((), ())), preferred_element_type=jnp.float32
            )
        for part in range(5):
            wide[pl.ds(2 * capacity + part, owners, stride=2 * stride), :] = table[
                part * owners : (part + 1) * owners
            ]
        move.wait()

        def place_rows(index, carry):
            for offset in range(unroll):
                token = index * unroll + offset
                wide[pl.ds(2 * targets[0, token], 2), :] = source[pl.ds(2 * token, 2), :]
            return carry

        lax.fori_loop(0, tokens // unroll, place_rows, 0)
        length = total // chunks
        copies = []
        for chunk in range(chunks):
            part = pl.ds(chunk * length, length)
            for half in range(2):
                packed[part, half * LANES : (half + 1) * LANES] = wide[
                    pl.ds(2 * chunk * length + half, length, stride=2), :
                ].astype(jnp.bfloat16)
            copies.append(
                pltpu.make_async_copy(packed.at[part], packed_hbm.at[part], done.at[2 + chunk])
            )
            if chunk:
                copies[-2].start()
        copies[-1].start()
        for copy in copies:
            copy.wait()

    return body


def sums_body(slots, per_cluster):
    def body(rows_ref, coarse_ref, fine_ref, coarse_out, fine_out, cand_out, norm_out,
             held_out, square_out, totals, counts, labels):
        columns = slots * per_cluster
        blocks, stride, _ = rows_ref.shape
        group = 16
        totals[...] = jnp.zeros_like(totals)
        counts[...] = jnp.zeros_like(counts)

        def read(block, carry):
            meta = rows_ref[block, LANES:stride, :].astype(jnp.float32)
            slot, fine = meta[0:1, :LANES], meta[0:1, LANES:]
            here = pl.ds(block, 1)
            labels[here, :] = ((slot - 1.0) * per_cluster + fine).astype(jnp.int32)
            held_out[here, :] = slot.astype(jnp.int32) - 1
            square_out[here, :] = (meta[1:2, :LANES] + meta[1:2, LANES:]) + meta[2:3, :LANES]
            return carry

        lax.fori_loop(0, blocks, read, 0, unroll=4)

        ids = iota((columns, LANES), 0).astype(jnp.int16)
        one, zero = jnp.bfloat16(1.0), jnp.bfloat16(0.0)

        def add(index, carry):
            hots = []
            count = jnp.zeros((columns, LANES), jnp.bfloat16)
            for offset in range(group):
                marks = labels[pl.ds(index * group + offset, 1), :]
                hot = jnp.where(ids == marks.astype(jnp.int16), one, zero)
                count = count + hot
                hots.append(hot)
            counts[...] += count.astype(jnp.float32)
            rows = jnp.concatenate(
                [rows_ref[index * group + offset, :LANES, :] for offset in range(group)], axis=0
            )
            totals[...] += jnp.dot(
                jnp.concatenate(hots, axis=1), rows, preferred_element_type=jnp.float32
            )
            return carry

        lax.fori_loop(0, blocks // group, add, 0)
        for slot in range(slots):
            part = pl.ds(slot * per_cluster, per_cluster)
            sum_f = totals[part, :]
            count_f = jnp.sum(counts[part, :], axis=1, keepdims=True)
            sum_c = jnp.sum(sum_f, axis=0, keepdims=True)
            count_c = jnp.sum(count_f, axis=0, keepdims=True)
            coarse = coarse_ref[slot : slot + 1, :]
            fine = fine_ref[part, :]
            over_c = 1.0 / (count_c + prior_weight)
            over_f = 1.0 / (count_f + prior_weight)
            for _ in range(PASSES):
                coarse = (sum_c + prior_weight * coarse) * over_c
                fine = (sum_f - count_f * coarse + prior_weight * fine) * over_f
            coarse_out[slot : slot + 1, :] = coarse
            fine_out[part, :] = fine
            cand = (coarse + fine).astype(jnp.bfloat16)
            value = cand.astype(jnp.float32)
            cand_out[part, :] = (value * -2.0).astype(jnp.bfloat16)
            norm_out[part, :] = jnp.broadcast_to(
                jnp.sum(value * value, axis=1, keepdims=True), (per_cluster, LANES)
            )

    return body


def distance_body(slots, per_cluster):
    def body(rows_ref, held_ref, square_ref, cand_ref, norm_ref, out_ref, powers):
        blocks = rows_ref.shape[0]
        pieces = out_ref.shape[0]
        quarter = per_cluster // pieces
        group, pair = blocks // CHUNKS, 2

        def one(index, carry):
            for first in range(0, group, pair):
                rows = jnp.concatenate(
                    [rows_ref[index * group + first + offset, :LANES, :] for offset in range(pair)],
                    axis=0,
                )
                cross = lax.dot_general(
                    cand_ref[...], rows, (((1,), (1,)), ((), ())),
                    preferred_element_type=jnp.float32,
                )
                for offset in range(pair):
                    block = index * group + first + offset
                    held = held_ref[pl.ds(block, 1), :]
                    value = jnp.zeros((per_cluster, LANES), jnp.float32)
                    for slot in range(slots):
                        part = slice(slot * per_cluster, (slot + 1) * per_cluster)
                        term = cross[part, offset * LANES : (offset + 1) * LANES] + norm_ref[part, :]
                        value = jnp.where(held == slot, term, value)
                    value = jnp.maximum(value + square_ref[pl.ds(block, 1), :], 0.0)
                    code, power = coded(value)
                    powers[pl.ds(block, 1), :] = power
                    for piece in range(pieces):
                        out_ref[piece, pl.ds(pl.multiple_of(block * quarter, quarter), quarter), :] = (
                            code[piece * quarter : (piece + 1) * quarter]
                        )
            return carry

        for chunk in range(CHUNKS):
            one(chunk, 0)
        for piece in range(pieces):
            out_ref[piece, blocks * quarter :, :] = powers[...].astype(jnp.int32).astype(jnp.int16)

    return body


def update_body(slots, per_cluster):
    sums = sums_body(slots, per_cluster)
    distances = distance_body(slots, per_cluster)

    def body(rows_ref, coarse_ref, fine_ref, coarse_out, fine_out, out_ref,
             totals, counts, labels, cand, norm, held, square, powers):
        sums(rows_ref, coarse_ref, fine_ref, coarse_out, fine_out, cand, norm, held, square,
             totals, counts, labels)
        distances(rows_ref, held, square, cand, norm, out_ref, powers)

    return body


def total_body(features):
    def body(got_ref, out_ref, scales):
        blocks, half, _ = out_ref.shape
        pieces = got_ref.shape[0]
        quarter = 2 * half
        for piece in range(pieces):
            scales[piece] = scale_of(got_ref[piece, blocks * quarter :, :])

        def one(block, carry):
            here = pl.ds(pl.multiple_of(block * quarter, quarter), quarter)
            value = decoded(got_ref[0, here, :], scales[0, pl.ds(block, 1), :])
            for piece in range(1, pieces):
                value = value + decoded(got_ref[piece, here, :], scales[piece, pl.ds(block, 1), :])
            out_ref[block] = floated(value * (1.0 / features))
            return carry

        lax.fori_loop(0, blocks, one, 0, unroll=8)

    return body


def pick_body(stride):
    def body(got_ref, owner_ref, target_ref, out_ref):
        owners, half, _ = got_ref.shape
        copies = out_ref.shape[0]
        groups = owner_ref.shape[1] // LANES

        def one(index, carry):
            here = pl.ds(pl.multiple_of(index * LANES, LANES), LANES)
            owner = owner_ref[:, here]
            place = target_ref[:, here] - owner * stride
            place = jnp.broadcast_to(place, (half, LANES))
            owner = jnp.broadcast_to(owner, (half, LANES))
            value = jnp.zeros((half, LANES), jnp.int32)
            for number in range(owners):
                found = jnp.take_along_axis(
                    got_ref[number], place, axis=1, mode="promise_in_bounds"
                )
                value = jnp.where(owner == number, found, value)
            for copy in range(copies):
                out_ref[copy, :, here] = value
            return carry

        lax.fori_loop(0, groups, one, 0, unroll=4)

    return body


def spread_body():
    def body(got_ref, out_ref):
        pieces, half, _ = got_ref.shape
        for piece in range(pieces):
            code = got_ref[piece]
            for part, value in enumerate((code & 65535, lax.shift_right_logical(code, 16))):
                start = (2 * piece + part) * half
                out_ref[start : start + half, :] = unfloated(value)

    return body


def arrange_body():
    def body(cluster_ref, rows_ref, out_ref):
        def move(index, carry):
            for offset in range(8):
                row = index * 8 + offset
                out_ref[pl.ds(cluster_ref[row], 1), :] = rows_ref[pl.ds(row, 1), :]
            return carry

        lax.fori_loop(0, rows_ref.shape[0] // 8, move, 0)

    return body


def shards(vectors, coarse_init, fine_init, owner_of, slot_in_owner, fine_in_cluster, slot_cluster):
    owners = lax.axis_size("dp")
    pieces = lax.axis_size("grp")
    tokens, width = vectors.shape
    slots, per_cluster, _ = fine_init.shape
    columns = slots * per_cluster
    features = width * pieces
    capacity = 2 * tokens // owners
    stride = capacity + 8
    quarter = per_cluster // pieces
    total = owners * capacity
    f32, bf16, i32 = jnp.float32, jnp.bfloat16, jnp.int32
    shape = jax.ShapeDtypeStruct

    i16 = jnp.int16
    owner = owner_of.reshape(1, tokens)
    slot, part = slot_in_owner.reshape(1, tokens), fine_in_cluster.reshape(1, tokens)
    target, send_rows = call(
        send_body(capacity, stride, 4, 32),
        (shape((1, tokens), i32), shape((owners * stride, width), bf16)),
        [VMEM, VMEM, VMEM, HBM],
        flops=400_000_000,
        scratch=[
            pltpu.VMEM((tokens, width), bf16),
            pltpu.VMEM((2 * tokens, LANES), f32),
            pltpu.VMEM((2 * owners * stride, LANES), f32),
            pltpu.VMEM((owners * stride, width), bf16),
            pltpu.SMEM((1, tokens), i32),
            pltpu.SemaphoreType.DMA((6,)),
        ],
        mem=56 << 20,
        outs=(VMEM, HBM),
    )(owner, slot, part, vectors)
    rows = exchanged(send_rows.reshape(owners, stride, width), "dp")
    bits = [bit for bit in (8, 4, 2, 32, 16, 1) if bit < owners]
    masks = [
        sum(bit for place, bit in enumerate(bits) if number >> place & 1) for number in range(owners)
    ]
    order = jnp.bitwise_xor(jnp.array(masks, i32), lax.axis_index("dp"))
    cluster_at = slot_cluster.reshape(owners, slots)[order].reshape(owners * slots)
    mine = lax.dynamic_slice_in_dim(slot_cluster, lax.axis_index("dp") * slots, slots, 0)
    coarse_mine, fine, partial = call(
        update_body(slots, per_cluster),
        (
            shape((slots, width), f32),
            shape((columns, width), f32),
            shape((pieces, owners * quarter + owners, capacity), i16),
        ),
        [VMEM] * 3,
        flops=4 * total * columns * width,
        scratch=[
            pltpu.VMEM((columns, width), f32),
            pltpu.VMEM((columns, LANES), f32),
            pltpu.VMEM((owners, LANES), i32),
            pltpu.VMEM((columns, width), bf16),
            pltpu.VMEM((columns, LANES), f32),
            pltpu.VMEM((owners, LANES), i32),
            pltpu.VMEM((owners, LANES), f32),
            pltpu.VMEM((owners, LANES), f32),
        ],
        mem=40 << 20,
    )(rows, coarse_init[mine], fine_init.reshape(columns, width))

    gathered = coarse_mine
    for bit in bits:
        other = lax.ppermute(gathered, "dp", [(i, i ^ bit) for i in range(owners)])
        gathered = jnp.concatenate([gathered, other], axis=0)

    arrived = exchanged(partial, "grp")
    share = call(
        total_body(features),
        shape((owners, quarter // 2, capacity), i32),
        [VMEM],
        flops=2_000_000_000,
        scratch=[pltpu.VMEM((pieces, owners, LANES), f32)],
    )(arrived)
    returned = exchanged(share, "dp")
    spread = call(
        pick_body(stride),
        shape((pieces, quarter // 2, tokens), i32),
        [VMEM] * 3,
        flops=4_000_000_000,
    )(returned, owner, target)
    codes = exchanged(spread, "grp")
    coarse_out = call(
        arrange_body(),
        shape((owners * slots, width), f32),
        [SMEM, VMEM],
        flops=2_000_000_000,
    )(cluster_at, gathered)
    distances = call(
        spread_body(), shape((per_cluster, tokens), f32), [VMEM], flops=10_000_000
    )(codes)
    return (coarse_out, fine.reshape(slots, per_cluster, width), distances)


def solution(mesh):
    return jax.shard_map(
        shards,
        mesh=mesh,
        in_specs=(
            P("dp", "grp"),
            P(None, "grp"),
            P("dp", None, "grp"),
            P("dp", None),
            P("dp"),
            P("dp"),
            P(),
        ),
        out_specs=(P(None, "grp"), P("dp", None, "grp"), P(None, "dp")),
        check_vma=False,
    )
```

```python
import jax
import jax.numpy as jnp
from jax import lax
from jax.experimental import pallas as pl
from jax.experimental.pallas import tpu as pltpu
from jax.sharding import PartitionSpec as P


PASSES = 2
LANES = 128
CHUNKS = 4


prior_weight = 2.0

VMEM = pl.BlockSpec(memory_space=pltpu.VMEM)
SMEM = pl.BlockSpec(memory_space=pltpu.SMEM)
HBM = pl.BlockSpec(memory_space=pl.ANY)


def call(body, out_shape, ins, flops, scratch=(), mem=16 << 20, outs=None):
    return pl.pallas_call(
        body,
        out_shape=out_shape,
        in_specs=ins,
        out_specs=outs or jax.tree.map(lambda _: VMEM, out_shape),
        scratch_shapes=list(scratch),
        compiler_params=pltpu.CompilerParams(vmem_limit_bytes=mem),
        cost_estimate=pl.CostEstimate(flops=flops, bytes_accessed=4 << 20, transcendentals=0),
    )


def exchanged(array, axis):
    return lax.all_to_all(array, axis, split_axis=0, concat_axis=0, tiled=True)


def iota(shape, dim):
    return lax.broadcasted_iota(jnp.int32, shape, dim)


def digits(value):
    first = value.astype(jnp.bfloat16).astype(jnp.float32)
    rest = value - first
    second = rest.astype(jnp.bfloat16).astype(jnp.float32)
    return first, second, rest - second


def coded(value):
    top = jnp.max(value, axis=0, keepdims=True)
    power = jnp.ceil(jnp.log2(jnp.maximum(top, 1e-30)))
    code = jnp.minimum(jnp.round(value * jnp.exp2(16.0 - power)), 65535.0) - 32768.0
    return code.astype(jnp.int32).astype(jnp.int16), power


def decoded(code, scale):
    return (code.astype(jnp.int32).astype(jnp.float32) + 32768.0) * scale


def scale_of(power):
    return jnp.exp2(power.astype(jnp.int32).astype(jnp.float32) - 16.0)


def floated(value):
    power = jnp.floor(jnp.log2(jnp.maximum(value, 2.0**-21)))
    power = jnp.clip(power, -21.0, 9.0)
    code = 2048.0 * (power + 21.0) + jnp.round(value * jnp.exp2(-power) * 2048.0)
    code = jnp.minimum(code, 65535.0).astype(jnp.int32)
    half = value.shape[0] // 2
    return code[:half] | (code[half:] << 16)


def unfloated(code):
    octave = jnp.maximum((code >> 11) - 1, 0)
    mantissa = (code - (octave << 11)).astype(jnp.float32)
    return mantissa * jnp.exp2(octave.astype(jnp.float32) - 32.0)


def send_body(capacity, stride, chunks, unroll):
    def body(owner_ref, slot_ref, fine_ref, rows_hbm, target_ref, packed_hbm,
             rows, source, wide, packed, targets, done):
        tokens = rows.shape[0]
        total = packed.shape[0]
        owners = total // stride
        step = 256
        load = pltpu.make_async_copy(rows_hbm, rows, done.at[0])
        load.start()
        upper = (iota((step, step), 0) < iota((step, step), 1)).astype(jnp.bfloat16)
        carry = jnp.zeros((owners, 1), jnp.float32)
        for start in range(0, tokens, step):
            owner = owner_ref[:, start : start + step]
            hot = (iota((owners, step), 0) == owner).astype(jnp.float32)
            before = carry + jnp.dot(
                hot.astype(jnp.bfloat16), upper, preferred_element_type=jnp.float32
            )
            place = jnp.sum(hot * before, axis=0, keepdims=True).astype(jnp.int32)
            carry = carry + jnp.sum(hot, axis=1, keepdims=True)
            target_ref[:, start : start + step] = owner * stride + place
        wide[...] = jnp.zeros_like(wide)
        move = pltpu.make_async_copy(target_ref, targets, done.at[1])
        move.start()
        load.wait()
        table = jnp.zeros((5 * owners, capacity), jnp.float32)
        for start in range(0, tokens, step):
            square = jnp.zeros((LANES, step), jnp.float32)
            for half in range(2):
                value = rows[
                    start : start + step, half * LANES : (half + 1) * LANES
                ].astype(jnp.float32)
                source[pl.ds(2 * start + half, step, stride=2), :] = value
                square = square + (value * value).T
            owner = owner_ref[:, start : start + step]
            place = target_ref[:, start : start + step] - owner * stride
            hot = (iota((owners, step), 0) == owner).astype(jnp.float32)
            at_place = (iota((capacity, step), 0) == place).astype(jnp.bfloat16)
            slot = slot_ref[:, start : start + step].astype(jnp.float32)
            fine = fine_ref[:, start : start + step].astype(jnp.float32)
            squares = digits(jnp.sum(square, axis=0, keepdims=True))
            parts = jnp.concatenate(
                [hot * value for value in (slot + 1.0, fine, *squares)], axis=0
            ).astype(jnp.bfloat16)
            table = table + lax.dot_general(
                parts, at_place, (((1,), (1,)), ((), ())), preferred_element_type=jnp.float32
            )
        for part in range(5):
            wide[pl.ds(2 * capacity + part, owners, stride=2 * stride), :] = table[
                part * owners : (part + 1) * owners
            ]
        move.wait()

        def place_rows(index, carry):
            for offset in range(unroll):
                token = index * unroll + offset
                wide[pl.ds(2 * targets[0, token], 2), :] = source[pl.ds(2 * token, 2), :]
            return carry

        lax.fori_loop(0, tokens // unroll, place_rows, 0)
        length = total // chunks
        copies = []
        for chunk in range(chunks):
            part = pl.ds(chunk * length, length)
            for half in range(2):
                packed[part, half * LANES : (half + 1) * LANES] = wide[
                    pl.ds(2 * chunk * length + half, length, stride=2), :
                ].astype(jnp.bfloat16)
            copies.append(
                pltpu.make_async_copy(packed.at[part], packed_hbm.at[part], done.at[2 + chunk])
            )
            if chunk:
                copies[-2].start()
        copies[-1].start()
        for copy in copies:
            copy.wait()

    return body


def sums_body(slots, per_cluster):
    def body(rows_ref, coarse_ref, fine_ref, coarse_out, fine_out, cand_out, norm_out,
             held_out, square_out, totals, counts, labels):
        columns = slots * per_cluster
        blocks, stride, _ = rows_ref.shape
        group = 16
        totals[...] = jnp.zeros_like(totals)
        counts[...] = jnp.zeros_like(counts)

        def read(block, carry):
            meta = rows_ref[block, LANES:stride, :].astype(jnp.float32)
            slot, fine = meta[0:1, :LANES], meta[0:1, LANES:]
            here = pl.ds(block, 1)
            labels[here, :] = ((slot - 1.0) * per_cluster + fine).astype(jnp.int32)
            held_out[here, :] = slot.astype(jnp.int32) - 1
            square_out[here, :] = (meta[1:2, :LANES] + meta[1:2, LANES:]) + meta[2:3, :LANES]
            return carry

        lax.fori_loop(0, blocks, read, 0, unroll=4)

        ids = iota((columns, LANES), 0).astype(jnp.int16)
        one, zero = jnp.bfloat16(1.0), jnp.bfloat16(0.0)

        def add(index, carry):
            hots = []
            count = jnp.zeros((columns, LANES), jnp.bfloat16)
            for offset in range(group):
                marks = labels[pl.ds(index * group + offset, 1), :]
                hot = jnp.where(ids == marks.astype(jnp.int16), one, zero)
                count = count + hot
                hots.append(hot)
            counts[...] += count.astype(jnp.float32)
            rows = jnp.concatenate(
                [rows_ref[index * group + offset, :LANES, :] for offset in range(group)], axis=0
            )
            totals[...] += jnp.dot(
                jnp.concatenate(hots, axis=1), rows, preferred_element_type=jnp.float32
            )
            return carry

        lax.fori_loop(0, blocks // group, add, 0)
        for slot in range(slots):
            part = pl.ds(slot * per_cluster, per_cluster)
            sum_f = totals[part, :]
            count_f = jnp.sum(counts[part, :], axis=1, keepdims=True)
            sum_c = jnp.sum(sum_f, axis=0, keepdims=True)
            count_c = jnp.sum(count_f, axis=0, keepdims=True)
            coarse = coarse_ref[slot : slot + 1, :]
            fine = fine_ref[part, :]
            over_c = 1.0 / (count_c + prior_weight)
            over_f = 1.0 / (count_f + prior_weight)
            for _ in range(PASSES):
                coarse = (sum_c + prior_weight * coarse) * over_c
                fine = (sum_f - count_f * coarse + prior_weight * fine) * over_f
            coarse_out[slot : slot + 1, :] = coarse
            fine_out[part, :] = fine
            cand = (coarse + fine).astype(jnp.bfloat16)
            value = cand.astype(jnp.float32)
            cand_out[part, :] = (value * -2.0).astype(jnp.bfloat16)
            norm_out[part, :] = jnp.broadcast_to(
                jnp.sum(value * value, axis=1, keepdims=True), (per_cluster, LANES)
            )

    return body


def distance_body(slots, per_cluster):
    def body(rows_ref, held_ref, square_ref, cand_ref, norm_ref, out_ref, powers):
        blocks = rows_ref.shape[0]
        pieces = out_ref.shape[0]
        quarter = per_cluster // pieces
        group, pair = blocks // CHUNKS, 2

        def one(index, carry):
            for first in range(0, group, pair):
                rows = jnp.concatenate(
                    [rows_ref[index * group + first + offset, :LANES, :] for offset in range(pair)],
                    axis=0,
                )
                cross = lax.dot_general(
                    cand_ref[...], rows, (((1,), (1,)), ((), ())),
                    preferred_element_type=jnp.float32,
                )
                for offset in range(pair):
                    block = index * group + first + offset
                    held = held_ref[pl.ds(block, 1), :]
                    value = jnp.zeros((per_cluster, LANES), jnp.float32)
                    for slot in range(slots):
                        part = slice(slot * per_cluster, (slot + 1) * per_cluster)
                        term = cross[part, offset * LANES : (offset + 1) * LANES] + norm_ref[part, :]
                        value = jnp.where(held == slot, term, value)
                    value = jnp.maximum(value + square_ref[pl.ds(block, 1), :], 0.0)
                    code, power = coded(value)
                    powers[pl.ds(block, 1), :] = power
                    for piece in range(pieces):
                        out_ref[piece, pl.ds(pl.multiple_of(block * quarter, quarter), quarter), :] = (
                            code[piece * quarter : (piece + 1) * quarter]
                        )
            return carry

        for chunk in range(CHUNKS):
            one(chunk, 0)
        for piece in range(pieces):
            out_ref[piece, blocks * quarter :, :] = powers[...].astype(jnp.int32).astype(jnp.int16)

    return body


def update_body(slots, per_cluster):
    sums = sums_body(slots, per_cluster)
    distances = distance_body(slots, per_cluster)

    def body(rows_ref, coarse_ref, fine_ref, coarse_out, fine_out, out_ref,
             totals, counts, labels, cand, norm, held, square, powers):
        sums(rows_ref, coarse_ref, fine_ref, coarse_out, fine_out, cand, norm, held, square,
             totals, counts, labels)
        distances(rows_ref, held, square, cand, norm, out_ref, powers)

    return body


def total_body(features):
    def body(got_ref, out_ref, scales):
        blocks, half, _ = out_ref.shape
        pieces = got_ref.shape[0]
        quarter = 2 * half
        for piece in range(pieces):
            scales[piece] = scale_of(got_ref[piece, blocks * quarter :, :])

        def one(block, carry):
            here = pl.ds(pl.multiple_of(block * quarter, quarter), quarter)
            value = decoded(got_ref[0, here, :], scales[0, pl.ds(block, 1), :])
            for piece in range(1, pieces):
                value = value + decoded(got_ref[piece, here, :], scales[piece, pl.ds(block, 1), :])
            out_ref[block] = floated(value * (1.0 / features))
            return carry

        lax.fori_loop(0, blocks, one, 0, unroll=8)

    return body


def pick_body(stride):
    def body(got_ref, owner_ref, target_ref, out_ref):
        owners, half, _ = got_ref.shape
        copies = out_ref.shape[0]
        groups = owner_ref.shape[1] // LANES

        def one(index, carry):
            here = pl.ds(pl.multiple_of(index * LANES, LANES), LANES)
            owner = owner_ref[:, here]
            place = target_ref[:, here] - owner * stride
            place = jnp.broadcast_to(place, (half, LANES))
            owner = jnp.broadcast_to(owner, (half, LANES))
            value = jnp.zeros((half, LANES), jnp.int32)
            for number in range(owners):
                found = jnp.take_along_axis(
                    got_ref[number], place, axis=1, mode="promise_in_bounds"
                )
                value = jnp.where(owner == number, found, value)
            for copy in range(copies):
                out_ref[copy, :, here] = value
            return carry

        lax.fori_loop(0, groups, one, 0, unroll=4)

    return body


def spread_body():
    def body(got_ref, out_ref):
        pieces, half, _ = got_ref.shape
        for piece in range(pieces):
            code = got_ref[piece]
            for part, value in enumerate((code & 65535, lax.shift_right_logical(code, 16))):
                start = (2 * piece + part) * half
                out_ref[start : start + half, :] = unfloated(value)

    return body


def arrange_body():
    def body(cluster_ref, first_ref, second_ref, out_ref):
        rows = first_ref.shape[0]

        def move(index, carry):
            for offset in range(8):
                row = index * 8 + offset
                out_ref[pl.ds(cluster_ref[row], 1), :] = first_ref[pl.ds(row, 1), :]
                out_ref[pl.ds(cluster_ref[row + rows], 1), :] = second_ref[pl.ds(row, 1), :]
            return carry

        lax.fori_loop(0, rows // 8, move, 0)

    return body


def shards(vectors, coarse_init, fine_init, owner_of, slot_in_owner, fine_in_cluster, slot_cluster):
    owners = lax.axis_size("dp")
    pieces = lax.axis_size("grp")
    tokens, width = vectors.shape
    slots, per_cluster, _ = fine_init.shape
    columns = slots * per_cluster
    features = width * pieces
    capacity = 2 * tokens // owners
    stride = capacity + 8
    quarter = per_cluster // pieces
    total = owners * capacity
    f32, bf16, i32 = jnp.float32, jnp.bfloat16, jnp.int32
    shape = jax.ShapeDtypeStruct

    i16 = jnp.int16
    owner = owner_of.reshape(1, tokens)
    slot, part = slot_in_owner.reshape(1, tokens), fine_in_cluster.reshape(1, tokens)
    target, send_rows = call(
        send_body(capacity, stride, 4, 32),
        (shape((1, tokens), i32), shape((owners * stride, width), bf16)),
        [VMEM, VMEM, VMEM, HBM],
        flops=400_000_000,
        scratch=[
            pltpu.VMEM((tokens, width), bf16),
            pltpu.VMEM((2 * tokens, LANES), f32),
            pltpu.VMEM((2 * owners * stride, LANES), f32),
            pltpu.VMEM((owners * stride, width), bf16),
            pltpu.SMEM((1, tokens), i32),
            pltpu.SemaphoreType.DMA((6,)),
        ],
        mem=56 << 20,
        outs=(VMEM, HBM),
    )(owner, slot, part, vectors)
    rows = exchanged(send_rows.reshape(owners, stride, width), "dp")
    bits = [bit for bit in (8, 4, 2, 32, 16, 1) if bit < owners]
    masks = [
        sum(bit for place, bit in enumerate(bits) if number >> place & 1) for number in range(owners)
    ]
    order = jnp.bitwise_xor(jnp.array(masks, i32), lax.axis_index("dp"))
    cluster_at = slot_cluster.reshape(owners, slots)[order].reshape(owners * slots)
    mine = lax.dynamic_slice_in_dim(slot_cluster, lax.axis_index("dp") * slots, slots, 0)
    coarse_mine, fine, partial = call(
        update_body(slots, per_cluster),
        (
            shape((slots, width), f32),
            shape((columns, width), f32),
            shape((pieces, owners * quarter + owners, capacity), i16),
        ),
        [VMEM] * 3,
        flops=4 * total * columns * width,
        scratch=[
            pltpu.VMEM((columns, width), f32),
            pltpu.VMEM((columns, LANES), f32),
            pltpu.VMEM((owners, LANES), i32),
            pltpu.VMEM((columns, width), bf16),
            pltpu.VMEM((columns, LANES), f32),
            pltpu.VMEM((owners, LANES), i32),
            pltpu.VMEM((owners, LANES), f32),
            pltpu.VMEM((owners, LANES), f32),
        ],
        mem=40 << 20,
    )(rows, coarse_init[mine], fine_init.reshape(columns, width))

    gathered = other = coarse_mine
    for hop, bit in enumerate(bits):
        if hop:
            gathered = lax.optimization_barrier(jnp.concatenate([gathered, other], axis=0))
        other = lax.ppermute(gathered, "dp", [(i, i ^ bit) for i in range(owners)])

    arrived = exchanged(partial, "grp")
    share = call(
        total_body(features),
        shape((owners, quarter // 2, capacity), i32),
        [VMEM],
        flops=2_000_000_000,
        scratch=[pltpu.VMEM((pieces, owners, LANES), f32)],
    )(arrived)
    returned = exchanged(share, "dp")
    spread = call(
        pick_body(stride),
        shape((pieces, quarter // 2, tokens), i32),
        [VMEM] * 3,
        flops=4_000_000_000,
    )(returned, owner, target)
    codes = exchanged(spread, "grp")
    coarse_out = call(
        arrange_body(),
        shape((owners * slots, width), f32),
        [SMEM, VMEM, VMEM],
        flops=2_000_000_000,
    )(cluster_at, gathered, other)
    distances = call(
        spread_body(), shape((per_cluster, tokens), f32), [VMEM], flops=10_000_000
    )(codes)
    return (coarse_out, fine.reshape(slots, per_cluster, width), distances)


def solution(mesh):
    return jax.shard_map(
        shards,
        mesh=mesh,
        in_specs=(
            P("dp", "grp"),
            P(None, "grp"),
            P("dp", None, "grp"),
            P("dp", None),
            P("dp"),
            P("dp"),
            P(),
        ),
        out_specs=(P(None, "grp"), P("dp", None, "grp"), P(None, "dp")),
        check_vma=False,
    )
```

```python
import jax
import jax.numpy as jnp
from jax import lax
from jax.experimental import pallas as pl
from jax.experimental.pallas import tpu as pltpu
from jax.sharding import PartitionSpec as P


PASSES = 2
LANES = 128
CHUNKS = 4


prior_weight = 2.0

VMEM = pl.BlockSpec(memory_space=pltpu.VMEM)
SMEM = pl.BlockSpec(memory_space=pltpu.SMEM)
HBM = pl.BlockSpec(memory_space=pl.ANY)


def call(body, out_shape, ins, flops, scratch=(), mem=16 << 20, outs=None):
    return pl.pallas_call(
        body,
        out_shape=out_shape,
        in_specs=ins,
        out_specs=outs or jax.tree.map(lambda _: VMEM, out_shape),
        scratch_shapes=list(scratch),
        compiler_params=pltpu.CompilerParams(vmem_limit_bytes=mem),
        cost_estimate=pl.CostEstimate(flops=flops, bytes_accessed=4 << 20, transcendentals=0),
    )


def exchanged(array, axis):
    return lax.all_to_all(array, axis, split_axis=0, concat_axis=0, tiled=True)


def iota(shape, dim):
    return lax.broadcasted_iota(jnp.int32, shape, dim)


def digits(value):
    first = value.astype(jnp.bfloat16).astype(jnp.float32)
    rest = value - first
    second = rest.astype(jnp.bfloat16).astype(jnp.float32)
    return first, second, rest - second


def coded(value):
    top = jnp.max(value, axis=0, keepdims=True)
    power = jnp.ceil(jnp.log2(jnp.maximum(top, 1e-30)))
    code = jnp.minimum(jnp.round(value * jnp.exp2(16.0 - power)), 65535.0) - 32768.0
    return code.astype(jnp.int32).astype(jnp.int16), power


def decoded(code, scale):
    return (code.astype(jnp.int32).astype(jnp.float32) + 32768.0) * scale


def scale_of(power):
    return jnp.exp2(power.astype(jnp.int32).astype(jnp.float32) - 16.0)


def floated(value):
    power = jnp.floor(jnp.log2(jnp.maximum(value, 2.0**-21)))
    power = jnp.clip(power, -21.0, 9.0)
    code = 2048.0 * (power + 21.0) + jnp.round(value * jnp.exp2(-power) * 2048.0)
    code = jnp.minimum(code, 65535.0).astype(jnp.int32)
    half = value.shape[0] // 2
    return code[:half] | (code[half:] << 16)


def unfloated(code):
    octave = jnp.maximum((code >> 11) - 1, 0)
    mantissa = (code - (octave << 11)).astype(jnp.float32)
    return mantissa * jnp.exp2(octave.astype(jnp.float32) - 32.0)


def send_body(capacity, stride, chunks, unroll):
    def body(owner_ref, slot_ref, fine_ref, rows_hbm, target_ref, packed_hbm,
             rows, source, wide, packed, targets, done):
        tokens = rows.shape[0]
        total = packed.shape[0]
        owners = total // stride
        step = 256
        load = pltpu.make_async_copy(rows_hbm, rows, done.at[0])
        load.start()
        upper = (iota((step, step), 0) < iota((step, step), 1)).astype(jnp.bfloat16)
        carry = jnp.zeros((owners, 1), jnp.float32)
        for start in range(0, tokens, step):
            owner = owner_ref[:, start : start + step]
            hot = (iota((owners, step), 0) == owner).astype(jnp.float32)
            before = carry + jnp.dot(
                hot.astype(jnp.bfloat16), upper, preferred_element_type=jnp.float32
            )
            place = jnp.sum(hot * before, axis=0, keepdims=True).astype(jnp.int32)
            carry = carry + jnp.sum(hot, axis=1, keepdims=True)
            target_ref[:, start : start + step] = owner * stride + place
        wide[...] = jnp.zeros_like(wide)
        move = pltpu.make_async_copy(target_ref, targets, done.at[1])
        move.start()
        load.wait()
        table = jnp.zeros((5 * owners, capacity), jnp.float32)
        for start in range(0, tokens, step):
            square = jnp.zeros((LANES, step), jnp.float32)
            for half in range(2):
                value = rows[
                    start : start + step, half * LANES : (half + 1) * LANES
                ].astype(jnp.float32)
                source[pl.ds(2 * start + half, step, stride=2), :] = value
                square = square + (value * value).T
            owner = owner_ref[:, start : start + step]
            place = target_ref[:, start : start + step] - owner * stride
            hot = (iota((owners, step), 0) == owner).astype(jnp.float32)
            at_place = (iota((capacity, step), 0) == place).astype(jnp.bfloat16)
            slot = slot_ref[:, start : start + step].astype(jnp.float32)
            fine = fine_ref[:, start : start + step].astype(jnp.float32)
            squares = digits(jnp.sum(square, axis=0, keepdims=True))
            parts = jnp.concatenate(
                [hot * value for value in (slot + 1.0, fine, *squares)], axis=0
            ).astype(jnp.bfloat16)
            table = table + lax.dot_general(
                parts, at_place, (((1,), (1,)), ((), ())), preferred_element_type=jnp.float32
            )
        for part in range(5):
            wide[pl.ds(2 * capacity + part, owners, stride=2 * stride), :] = table[
                part * owners : (part + 1) * owners
            ]
        move.wait()

        def place_rows(index, carry):
            for offset in range(unroll):
                token = index * unroll + offset
                wide[pl.ds(2 * targets[0, token], 2), :] = source[pl.ds(2 * token, 2), :]
            return carry

        lax.fori_loop(0, tokens // unroll, place_rows, 0)
        length = total // chunks
        copies = []
        for chunk in range(chunks):
            part = pl.ds(chunk * length, length)
            for half in range(2):
                packed[part, half * LANES : (half + 1) * LANES] = wide[
                    pl.ds(2 * chunk * length + half, length, stride=2), :
                ].astype(jnp.bfloat16)
            copies.append(
                pltpu.make_async_copy(packed.at[part], packed_hbm.at[part], done.at[2 + chunk])
            )
            if chunk:
                copies[-2].start()
        copies[-1].start()
        for copy in copies:
            copy.wait()

    return body


def sums_body(slots, per_cluster):
    def body(rows_ref, coarse_ref, fine_ref, coarse_out, fine_out, cand_out, norm_out,
             held_out, square_out, totals, counts, labels):
        columns = slots * per_cluster
        blocks, stride, _ = rows_ref.shape
        group = 16
        totals[...] = jnp.zeros_like(totals)
        counts[...] = jnp.zeros_like(counts)

        def read(block, carry):
            meta = rows_ref[block, LANES:stride, :].astype(jnp.float32)
            slot, fine = meta[0:1, :LANES], meta[0:1, LANES:]
            here = pl.ds(block, 1)
            labels[here, :] = ((slot - 1.0) * per_cluster + fine).astype(jnp.int32)
            held_out[here, :] = slot.astype(jnp.int32) - 1
            square_out[here, :] = (meta[1:2, :LANES] + meta[1:2, LANES:]) + meta[2:3, :LANES]
            return carry

        lax.fori_loop(0, blocks, read, 0, unroll=8)

        ids = iota((columns, LANES), 0).astype(jnp.int16)
        one, zero = jnp.bfloat16(1.0), jnp.bfloat16(0.0)

        def add(index, carry):
            hots = []
            count = jnp.zeros((columns, LANES), jnp.bfloat16)
            for offset in range(group):
                marks = labels[pl.ds(index * group + offset, 1), :]
                hot = jnp.where(ids == marks.astype(jnp.int16), one, zero)
                count = count + hot
                hots.append(hot)
            counts[...] += count.astype(jnp.float32)
            rows = jnp.concatenate(
                [rows_ref[index * group + offset, :LANES, :] for offset in range(group)], axis=0
            )
            totals[...] += jnp.dot(
                jnp.concatenate(hots, axis=1), rows, preferred_element_type=jnp.float32
            )
            return carry

        lax.fori_loop(0, blocks // group, add, 0)
        for slot in range(slots):
            part = pl.ds(slot * per_cluster, per_cluster)
            sum_f = totals[part, :]
            count_f = jnp.sum(counts[part, :], axis=1, keepdims=True)
            sum_c = jnp.sum(sum_f, axis=0, keepdims=True)
            count_c = jnp.sum(count_f, axis=0, keepdims=True)
            coarse = coarse_ref[slot : slot + 1, :]
            fine = fine_ref[part, :]
            over_c = 1.0 / (count_c + prior_weight)
            over_f = 1.0 / (count_f + prior_weight)
            for _ in range(PASSES):
                coarse = (sum_c + prior_weight * coarse) * over_c
                fine = (sum_f - count_f * coarse + prior_weight * fine) * over_f
            coarse_out[slot : slot + 1, :] = coarse
            fine_out[part, :] = fine
            cand = (coarse + fine).astype(jnp.bfloat16)
            value = cand.astype(jnp.float32)
            cand_out[part, :] = (value * -2.0).astype(jnp.bfloat16)
            norm_out[part, :] = jnp.broadcast_to(
                jnp.sum(value * value, axis=1, keepdims=True), (per_cluster, LANES)
            )

    return body


def distance_body(slots, per_cluster):
    def body(rows_ref, held_ref, square_ref, cand_ref, norm_ref, out_ref, powers):
        blocks = rows_ref.shape[0]
        pieces = out_ref.shape[0]
        quarter = per_cluster // pieces
        group, pair = blocks // CHUNKS, 2

        def one(index, carry):
            for first in range(0, group, pair):
                rows = jnp.concatenate(
                    [rows_ref[index * group + first + offset, :LANES, :] for offset in range(pair)],
                    axis=0,
                )
                cross = lax.dot_general(
                    cand_ref[...], rows, (((1,), (1,)), ((), ())),
                    preferred_element_type=jnp.float32,
                )
                for offset in range(pair):
                    block = index * group + first + offset
                    held = held_ref[pl.ds(block, 1), :]
                    value = jnp.zeros((per_cluster, LANES), jnp.float32)
                    for slot in range(slots):
                        part = slice(slot * per_cluster, (slot + 1) * per_cluster)
                        term = cross[part, offset * LANES : (offset + 1) * LANES] + norm_ref[part, :]
                        value = jnp.where(held == slot, term, value)
                    value = jnp.maximum(value + square_ref[pl.ds(block, 1), :], 0.0)
                    code, power = coded(value)
                    powers[pl.ds(block, 1), :] = power
                    for piece in range(pieces):
                        out_ref[piece, pl.ds(pl.multiple_of(block * quarter, quarter), quarter), :] = (
                            code[piece * quarter : (piece + 1) * quarter]
                        )
            return carry

        for chunk in range(CHUNKS):
            one(chunk, 0)
        for piece in range(pieces):
            out_ref[piece, blocks * quarter :, :] = powers[...].astype(jnp.int32).astype(jnp.int16)

    return body


def update_body(slots, per_cluster):
    sums = sums_body(slots, per_cluster)
    distances = distance_body(slots, per_cluster)

    def body(rows_ref, coarse_ref, fine_ref, coarse_out, fine_out, out_ref,
             totals, counts, labels, cand, norm, held, square, powers):
        sums(rows_ref, coarse_ref, fine_ref, coarse_out, fine_out, cand, norm, held, square,
             totals, counts, labels)
        distances(rows_ref, held, square, cand, norm, out_ref, powers)

    return body


def total_body(features):
    def body(got_ref, out_ref, scales):
        blocks, half, _ = out_ref.shape
        pieces = got_ref.shape[0]
        quarter = 2 * half
        for piece in range(pieces):
            scales[piece] = scale_of(got_ref[piece, blocks * quarter :, :])

        def one(block, carry):
            here = pl.ds(pl.multiple_of(block * quarter, quarter), quarter)
            value = decoded(got_ref[0, here, :], scales[0, pl.ds(block, 1), :])
            for piece in range(1, pieces):
                value = value + decoded(got_ref[piece, here, :], scales[piece, pl.ds(block, 1), :])
            out_ref[block] = floated(value * (1.0 / features))
            return carry

        lax.fori_loop(0, blocks, one, 0, unroll=8)

    return body


def pick_body(stride):
    def body(got_ref, owner_ref, target_ref, out_ref):
        owners, half, _ = got_ref.shape
        copies = out_ref.shape[0]
        groups = owner_ref.shape[1] // LANES

        def one(index, carry):
            here = pl.ds(pl.multiple_of(index * LANES, LANES), LANES)
            owner = owner_ref[:, here]
            place = target_ref[:, here] - owner * stride
            place = jnp.broadcast_to(place, (half, LANES))
            owner = jnp.broadcast_to(owner, (half, LANES))
            value = jnp.zeros((half, LANES), jnp.int32)
            for number in range(owners):
                found = jnp.take_along_axis(
                    got_ref[number], place, axis=1, mode="promise_in_bounds"
                )
                value = jnp.where(owner == number, found, value)
            for copy in range(copies):
                out_ref[copy, :, here] = value
            return carry

        lax.fori_loop(0, groups, one, 0, unroll=8)

    return body


def spread_body():
    def body(got_ref, out_ref):
        pieces, half, _ = got_ref.shape
        for piece in range(pieces):
            code = got_ref[piece]
            for part, value in enumerate((code & 65535, lax.shift_right_logical(code, 16))):
                start = (2 * piece + part) * half
                out_ref[start : start + half, :] = unfloated(value)

    return body


def arrange_body():
    def body(cluster_ref, first_ref, second_ref, out_ref):
        rows = first_ref.shape[0]

        def move(index, carry):
            for offset in range(8):
                row = index * 8 + offset
                out_ref[pl.ds(cluster_ref[row], 1), :] = first_ref[pl.ds(row, 1), :]
                out_ref[pl.ds(cluster_ref[row + rows], 1), :] = second_ref[pl.ds(row, 1), :]
            return carry

        lax.fori_loop(0, rows // 8, move, 0)

    return body


def shards(vectors, coarse_init, fine_init, owner_of, slot_in_owner, fine_in_cluster, slot_cluster):
    owners = lax.axis_size("dp")
    pieces = lax.axis_size("grp")
    tokens, width = vectors.shape
    slots, per_cluster, _ = fine_init.shape
    columns = slots * per_cluster
    features = width * pieces
    capacity = 2 * tokens // owners
    stride = capacity + 8
    quarter = per_cluster // pieces
    total = owners * capacity
    f32, bf16, i32 = jnp.float32, jnp.bfloat16, jnp.int32
    shape = jax.ShapeDtypeStruct

    i16 = jnp.int16
    owner = owner_of.reshape(1, tokens)
    slot, part = slot_in_owner.reshape(1, tokens), fine_in_cluster.reshape(1, tokens)
    target, send_rows = call(
        send_body(capacity, stride, 4, 64),
        (shape((1, tokens), i32), shape((owners * stride, width), bf16)),
        [VMEM, VMEM, VMEM, HBM],
        flops=400_000_000,
        scratch=[
            pltpu.VMEM((tokens, width), bf16),
            pltpu.VMEM((2 * tokens, LANES), f32),
            pltpu.VMEM((2 * owners * stride, LANES), f32),
            pltpu.VMEM((owners * stride, width), bf16),
            pltpu.SMEM((1, tokens), i32),
            pltpu.SemaphoreType.DMA((6,)),
        ],
        mem=56 << 20,
        outs=(VMEM, HBM),
    )(owner, slot, part, vectors)
    rows = exchanged(send_rows.reshape(owners, stride, width), "dp")
    bits = [bit for bit in (8, 4, 2, 32, 16, 1) if bit < owners]
    masks = [
        sum(bit for place, bit in enumerate(bits) if number >> place & 1) for number in range(owners)
    ]
    order = jnp.bitwise_xor(jnp.array(masks, i32), lax.axis_index("dp"))
    cluster_at = slot_cluster.reshape(owners, slots)[order].reshape(owners * slots)
    mine = lax.dynamic_slice_in_dim(slot_cluster, lax.axis_index("dp") * slots, slots, 0)
    coarse_mine, fine, partial = call(
        update_body(slots, per_cluster),
        (
            shape((slots, width), f32),
            shape((columns, width), f32),
            shape((pieces, owners * quarter + owners, capacity), i16),
        ),
        [VMEM] * 3,
        flops=4 * total * columns * width,
        scratch=[
            pltpu.VMEM((columns, width), f32),
            pltpu.VMEM((columns, LANES), f32),
            pltpu.VMEM((owners, LANES), i32),
            pltpu.VMEM((columns, width), bf16),
            pltpu.VMEM((columns, LANES), f32),
            pltpu.VMEM((owners, LANES), i32),
            pltpu.VMEM((owners, LANES), f32),
            pltpu.VMEM((owners, LANES), f32),
        ],
        mem=40 << 20,
    )(rows, coarse_init[mine], fine_init.reshape(columns, width))

    gathered = other = coarse_mine
    for hop, bit in enumerate(bits):
        if hop:
            gathered = lax.optimization_barrier(jnp.concatenate([gathered, other], axis=0))
        other = lax.ppermute(gathered, "dp", [(i, i ^ bit) for i in range(owners)])

    arrived = exchanged(partial, "grp")
    share = call(
        total_body(features),
        shape((owners, quarter // 2, capacity), i32),
        [VMEM],
        flops=2_000_000_000,
        scratch=[pltpu.VMEM((pieces, owners, LANES), f32)],
    )(arrived)
    returned = exchanged(share, "dp")
    spread = call(
        pick_body(stride),
        shape((pieces, quarter // 2, tokens), i32),
        [VMEM] * 3,
        flops=4_000_000_000,
    )(returned, owner, target)
    codes = exchanged(spread, "grp")
    coarse_out = call(
        arrange_body(),
        shape((owners * slots, width), f32),
        [SMEM, VMEM, VMEM],
        flops=2_000_000_000,
    )(cluster_at, gathered, other)
    distances = call(
        spread_body(), shape((per_cluster, tokens), f32), [VMEM], flops=10_000_000
    )(codes)
    return (coarse_out, fine.reshape(slots, per_cluster, width), distances)


def solution(mesh):
    return jax.shard_map(
        shards,
        mesh=mesh,
        in_specs=(
            P("dp", "grp"),
            P(None, "grp"),
            P("dp", None, "grp"),
            P("dp", None),
            P("dp"),
            P("dp"),
            P(),
        ),
        out_specs=(P(None, "grp"), P("dp", None, "grp"), P(None, "dp")),
        check_vma=False,
    )
```
